16 devices in a mesh: col: 2 (over z), row: 8 (over y, x, core).
Axes of the slice: x: 2, y: 2, z: 2, core: 2. Of those that a mesh axis runs over, the one named last changes fastest.
Arguments:
- hyper_params: float32 [3], replicated
- w_in: float32 [4, 2048, 5120], P(None, 'row', 'col')
- x_in: bfloat16 [4, 512, 2048], P(None, None, 'row')
- dy_in: bfloat16 [4, 512, 5120], P(None, None, 'col')
- row_in: float32 [4, 2048], P(None, 'row')
- col_in: float32 [4, 5120], P(None, 'col')
- w_out: float32 [4, 5120, 2048], P(None, 'col', 'row')
- x_out: bfloat16 [4, 512, 5120], P(None, None, 'col')
- dy_out: bfloat16 [4, 512, 2048], P(None, None, 'row')
- row_out: float32 [4, 5120], P(None, 'col')
- col_out: float32 [4, 2048], P(None, 'row')
Outputs:
- output 1: float32 [4, 2048, 5120], P(None, 'row', 'col')
- output 2: float32 [4, 2048], P(None, 'row')
- output 3: float32 [4, 5120], P(None, 'col')
- output 4: float32 [4, 5120, 2048], P(None, 'col', 'row')
- output 5: float32 [4, 5120], P(None, 'col')
- output 6: float32 [4, 2048], P(None, 'row')
All inputs are finite; a program needn't handle non-finite values.
Results may differ from the reference program's by a relative error of at most 0.001.
Values are sent between devices in bfloat16 or wider.
A program may use at most 1 GiB of HBM per device.

```python
import jax
import jax.numpy as jnp
from jax import lax

LAYERS = 4
TOKENS = 512
D_MODEL = 2048
D_FF = 5120
LATENT_RANK = 4
EPS_ONE = 1e-30
EPS_TWO = 1e-3
TWO_PI = 6.283185307179586


def profile(draw_key, length):
    phase_off = jax.random.uniform(draw_key, (LAYERS, LATENT_RANK, 1), jnp.float32) * TWO_PI
    freq_rank = (jnp.arange(LATENT_RANK) + 1).astype(jnp.float32)[None, :, None]
    position = (jnp.arange(length).astype(jnp.float32) / length)[None, None, :]
    return 1.0 + 0.9 * jnp.sin(TWO_PI * freq_rank * position + phase_off)


def draw_matrix(draw_key, n_rows, n_cols):
    sub_keys = jax.random.split(draw_key, 10)
    latent = jax.random.normal(sub_keys[0], (LAYERS, TOKENS, LATENT_RANK), jnp.float32)
    load_rows = jax.random.normal(sub_keys[1], (LAYERS, LATENT_RANK, n_rows), jnp.float32) * profile(sub_keys[2], n_rows)
    load_cols = jax.random.normal(sub_keys[3], (LAYERS, LATENT_RANK, n_cols), jnp.float32) * profile(sub_keys[4], n_cols)
    x_act = jnp.einsum('ltk,lkm->ltm', latent, load_rows) + jax.random.normal(sub_keys[5], (LAYERS, TOKENS, n_rows), jnp.float32)
    dy_act = (jnp.einsum('ltk,lkn->ltn', latent, load_cols) + jax.random.normal(sub_keys[6], (LAYERS, TOKENS, n_cols), jnp.float32)) / TOKENS
    w_mat = jax.random.normal(sub_keys[7], (LAYERS, n_rows, n_cols), jnp.float32) * n_rows ** -0.5
    row_stat = 6.0 * jnp.exp(0.5 * jax.random.normal(sub_keys[8], (LAYERS, n_rows), jnp.float32))
    col_stat = 6.0 * jnp.exp(0.5 * jax.random.normal(sub_keys[9], (LAYERS, n_cols), jnp.float32))
    return w_mat, x_act.astype(jnp.bfloat16), dy_act.astype(jnp.bfloat16), row_stat, col_stat


def setup_inputs(seed: int = 0) -> dict:
    sub_keys = jax.random.split(jax.random.key(seed), 3)
    low_end = jnp.array([0.5, 0.5, 0.2], dtype=jnp.float32)
    span_width = jnp.array([0.3, 0.5, 0.2], dtype=jnp.float32)
    hyper_params = low_end + span_width * jax.random.uniform(sub_keys[0], (3,), jnp.float32)
    w_in, x_in, dy_in, row_in, col_in = draw_matrix(sub_keys[1], D_MODEL, D_FF)
    w_out, x_out, dy_out, row_out, col_out = draw_matrix(sub_keys[2], D_FF, D_MODEL)
    return {'hyper_params': hyper_params, 'w_in': w_in, 'x_in': x_in, 'dy_in': dy_in, 'row_in': row_in, 'col_in': col_in, 'w_out': w_out, 'x_out': x_out, 'dy_out': dy_out, 'row_out': row_out, 'col_out': col_out}


def adafactor_one(w_mat, x_act, dy_act, row_old, col_old, hyper_params):
    beta_two = hyper_params[0]
    rho_step = hyper_params[1]
    clip_max = hyper_params[2]
    grad_mat = jnp.dot(x_act.T, dy_act, preferred_element_type=jnp.float32)
    sq_grad = grad_mat * grad_mat + EPS_ONE
    row_new = beta_two * row_old + (1.0 - beta_two) * jnp.mean(sq_grad, axis=1)
    col_new = beta_two * col_old + (1.0 - beta_two) * jnp.mean(sq_grad, axis=0)
    row_mean = jnp.mean(row_new)
    update = grad_mat * lax.rsqrt((row_new / row_mean)[:, None] * col_new[None, :])
    upd_rms = jnp.sqrt(jnp.mean(update * update))
    w_rms = jnp.sqrt(jnp.mean(w_mat * w_mat))
    step_size = rho_step * jnp.maximum(EPS_TWO, w_rms) / jnp.maximum(1.0, upd_rms / clip_max)
    return w_mat - step_size * update, row_new, col_new


def reference(hyper_params, w_in, x_in, dy_in, row_in, col_in, w_out, x_out, dy_out, row_out, col_out):
    def one_layer(layer_args):
        w_first, x_first, dy_first, row_first, col_first, w_second, x_second, dy_second, row_second, col_second = layer_args
        in_result = adafactor_one(w_first, x_first, dy_first, row_first, col_first, hyper_params)
        out_result = adafactor_one(w_second, x_second, dy_second, row_second, col_second, hyper_params)
        return in_result + out_result
    results = lax.map(one_layer, (w_in, x_in, dy_in, row_in, col_in, w_out, x_out, dy_out, row_out, col_out))
    return (results[0], results[1], results[2], results[3], results[4], results[5])
```

```python
import functools

import jax
import jax.numpy as jnp
from jax import lax
from jax.experimental import pallas as pl
from jax.experimental.pallas import tpu as pltpu
from jax.sharding import PartitionSpec as P

EPS_ONE = 1e-30
EPS_TWO = 1e-3
LANE = 128
CHUNK = 256
MESH = pl.DeviceIdType.MESH
F32 = jnp.float32


def stats_kernel(dims, hyper_hbm, w_in, x_in, dy_in, row_in, col_in, w_out, x_out, dy_out, row_out, col_out,
                 grad, wv_in, wv_out, short_new, long_new, scal,
                 act_s, act_l, lhs_t, old_s_in, old_l_in, old_s_out, old_l_out, short_old, long_old,
                 long_buf, short_buf, fin_buf, racc, cacc, rscale, linv, pack, hyper_ref,
                 act_sem, w_sem, old_sem, long_send, long_recv, short_send, short_recv, fin_send, fin_recv):
    n_col, n_row, layers, ms, ml, d_model, d_hidden = dims
    n_dev = n_col * n_row
    sch, lch = ms // LANE, ml // LANE
    my_col = lax.axis_index('col')
    my_row = lax.axis_index('row')

    def act_copies(layer, kind):
        slot = 2 * lax.rem(layer, 2) + kind
        src_s = (x_in, dy_out)[kind]
        src_l = (dy_in, x_out)[kind]
        return (pltpu.make_async_copy(src_s.at[layer], act_s.at[slot], act_sem.at[slot, 0]),
                pltpu.make_async_copy(src_l.at[layer], act_l.at[slot], act_sem.at[slot, 1]))

    def w_copy(layer, kind):
        src = (w_in, w_out)[kind]
        dst = (wv_in, wv_out)[kind]
        return pltpu.make_async_copy(src.at[layer], dst.at[layer], w_sem.at[layer, kind])

    old_copies = [pltpu.make_async_copy(src, dst, old_sem.at[idx]) for idx, (src, dst) in enumerate(
        ((row_in, old_s_in), (col_in, old_l_in), (col_out, old_s_out), (row_out, old_l_out), (hyper_hbm, hyper_ref)))]

    for layer in range(2):
        for kind in range(2):
            for copy in act_copies(layer, kind):
                copy.start()
    for copy in old_copies:
        copy.start()

    barrier = pltpu.get_barrier_semaphore()

    def peer_of(step):
        lin = lax.rem(my_col * n_row + my_row + step, n_dev)
        return (lin // n_row, lax.rem(lin, n_row))

    for step in range(1, n_dev):
        pl.semaphore_signal(barrier, inc=1, device_id=peer_of(step), device_id_type=MESH)

    pack[...] = jnp.zeros_like(pack)
    for copy in old_copies:
        copy.wait()
    beta_two = hyper_ref[0]
    for kind, (src_s, src_l) in enumerate(((old_s_in, old_l_in), (old_s_out, old_l_out))):
        for layer in range(layers):
            for j in range(sch):
                short_old[2 * layer + kind, j:j + 1, :] = src_s[layer:layer + 1, j * LANE:(j + 1) * LANE]
            for j in range(lch):
                long_old[2 * layer + kind, j:j + 1, :] = src_l[layer:layer + 1, j * LANE:(j + 1) * LANE]
    pl.semaphore_wait(barrier, n_dev - 1)

    def long_copy(mat, step):
        peer = lax.rem(my_row + step, n_row)
        return pltpu.make_async_remote_copy(
            src_ref=long_buf.at[mat, my_row], dst_ref=long_buf.at[mat, my_row],
            send_sem=long_send.at[mat], recv_sem=long_recv.at[mat],
            device_id=(my_col, peer), device_id_type=MESH)

    def short_copy(mat):
        return pltpu.make_async_remote_copy(
            src_ref=short_buf.at[mat, my_col], dst_ref=short_buf.at[mat, my_col],
            send_sem=short_send.at[mat], recv_sem=short_recv.at[mat],
            device_id=(n_col - 1 - my_col, my_row), device_id_type=MESH)

    def form_grad(layer, kind):
        mat = 2 * layer + kind
        slot = 2 * lax.rem(layer, 2) + kind
        for copy in act_copies(layer, kind):
            copy.wait()
        lhs_t[...] = act_s[slot].T
        racc[...] = jnp.zeros_like(racc)

        def chunk(c, carry):
            cols = pl.ds(pl.multiple_of(c * CHUNK, CHUNK), CHUNK)
            g = jnp.dot(lhs_t[...], act_l[slot, :, cols], preferred_element_type=F32)
            grad[mat, :, cols] = g
            sq = g * g
            racc[...] += sq[:, :LANE] + sq[:, LANE:]
            cacc[:, cols] = jnp.sum(sq.reshape(ms // 8, 8, CHUNK), axis=0)
            return carry

        lax.fori_loop(0, ml // CHUNK, chunk, 0)
        for j in range(lch):
            long_buf[mat, my_row, j:j + 1, :] = jnp.sum(cacc[:, j * LANE:(j + 1) * LANE], axis=0, keepdims=True)
        for j in range(sch):
            part = racc[j * LANE:(j + 1) * LANE, :].T
            short_buf[mat, my_col, j:j + 1, :] = jnp.sum(part, axis=0, keepdims=True)
        for step in range(1, n_row):
            long_copy(mat, step).start()
        short_copy(mat).start()

    def put(lane, value):
        at = lax.broadcasted_iota(jnp.int32, (1, LANE), 1) == lane
        pack[...] += jnp.where(at, value, 0.0)

    def total(value):
        return jnp.sum(jnp.sum(value, axis=1, keepdims=True), axis=0, keepdims=True)

    def update_sq(layer, kind):
        mat = 2 * layer + kind
        pltpu.make_async_copy(long_buf.at[mat, pl.ds(0, n_row - 1)], long_buf.at[mat, pl.ds(0, n_row - 1)],
                              long_recv.at[mat]).wait()
        short_copy(mat).wait_recv()
        lsum = long_buf[mat, 0]
        for dev in range(1, n_row):
            lsum = lsum + long_buf[mat, dev]
        ssum = short_buf[mat, 0]
        for dev in range(1, n_col):
            ssum = ssum + short_buf[mat, dev]
        lnew = beta_two * long_old[mat] + (1.0 - beta_two) * (lsum * (1.0 / d_model) + EPS_ONE)
        snew = beta_two * short_old[mat] + (1.0 - beta_two) * (ssum * (1.0 / d_hidden) + EPS_ONE)
        long_new[mat] = lnew
        short_new[mat] = snew
        if kind == 0:
            rho = total(snew)
            rs = lax.rsqrt(snew / (rho * (1.0 / ms)))
            linv[...] = 1.0 / lnew
        else:
            rho = total(lnew)
            rs = lax.rsqrt(snew)
            linv[...] = (rho * (1.0 / ml)) / lnew
        for j in range(sch):
            rscale[j * LANE:(j + 1) * LANE, :] = jnp.broadcast_to(rs[j:j + 1, :], (LANE, LANE)).T

        def chunk(c, acc):
            scale = rscale[...]
            for h in range(CHUNK // LANE):
                j = c * (CHUNK // LANE) + h
                u = grad[mat, :, pl.ds(pl.multiple_of(j * LANE, LANE), LANE)] * scale
                part = jnp.sum((u * u).reshape(ms // 8, 8, LANE), axis=0)
                acc = acc + part * linv[pl.ds(j, 1), :]
            return acc

        acc = lax.fori_loop(0, ml // CHUNK, chunk, jnp.zeros((8, LANE), F32))
        put(mat, total(acc))
        put(mat + 2 * layers, rho)

    def weight_sq(layer, kind):
        mat = 2 * layer + kind
        w_copy(layer, kind).wait()
        ref = (wv_in, wv_out)[kind]
        rows, cols = ref.shape[1:]
        block = max(8, 8 * 8 * 20 * LANE // cols)

        def chunk(t, acc):
            v = ref[layer, pl.ds(pl.multiple_of(t * block, 8), block), :]
            v = v * v
            part = v[:, :LANE]
            for j in range(1, cols // LANE):
                part = part + v[:, j * LANE:(j + 1) * LANE]
            return acc + jnp.sum(part.reshape(block // 8, 8, LANE), axis=0)

        acc = lax.fori_loop(0, rows // block, chunk, jnp.zeros((8, LANE), F32))
        put(mat + 4 * layers, total(acc))

    def phase_one(layer, carry):
        for kind in range(2):
            form_grad(layer, kind)

            @pl.when(layer + 2 < layers)
            def _():
                for copy in act_copies(layer + 2, kind):
                    copy.start()

            w_copy(layer, kind).start()

        @pl.when(layer >= 2)
        def _():
            for kind in range(2):
                update_sq(layer - 2, kind)

        return carry

    lax.fori_loop(0, layers, phase_one, 0)

    def phase_two(layer, carry):
        @pl.when(layer >= layers - 2)
        def _():
            for kind in range(2):
                update_sq(layer, kind)

        for kind in range(2):
            weight_sq(layer, kind)
        return carry

    lax.fori_loop(0, layers, phase_two, 0)

    me = my_col * n_row + my_row
    fin_buf[me] = pack[...]

    def fin_copy(step):
        return pltpu.make_async_remote_copy(
            src_ref=fin_buf.at[me], dst_ref=fin_buf.at[me], send_sem=fin_send, recv_sem=fin_recv,
            device_id=peer_of(step), device_id_type=MESH)

    for step in range(1, n_dev):
        fin_copy(step).start()
    for mat in range(2 * layers):
        pltpu.make_async_copy(long_buf.at[mat, pl.ds(0, n_row - 1)], long_buf.at[mat, pl.ds(0, n_row - 1)],
                              long_send.at[mat]).wait()
        short_copy(mat).wait_send()
    others = fin_buf.at[pl.ds(0, n_dev - 1)]
    pltpu.make_async_copy(others, others, fin_send).wait()
    pltpu.make_async_copy(others, others, fin_recv).wait()

    lane = lax.broadcasted_iota(jnp.int32, (1, LANE), 1)
    is_in = lax.rem(lane, 2) == 0
    valid = lane < 2 * layers
    rho_sum = jnp.zeros((1, LANE), F32)
    w_sq = jnp.zeros((1, LANE), F32)
    for dev in range(n_dev):
        rho_sum = rho_sum + pltpu.roll(fin_buf[dev], LANE - 2 * layers, 1)
        w_sq = w_sq + pltpu.roll(fin_buf[dev], LANE - 4 * layers, 1)
    row_mean = rho_sum * jnp.where(is_in, 1.0 / (n_col * d_model), 1.0 / (n_row * d_hidden))
    row_mean = jnp.where(valid, row_mean, 1.0)
    upd_sq = jnp.zeros((1, LANE), F32)
    for dev in range(n_dev):
        sigma = pltpu.roll(fin_buf[dev], LANE - 2 * layers, 1) * jnp.where(is_in, 1.0 / ms, 1.0 / ml)
        upd_sq = upd_sq + fin_buf[dev] * (row_mean / jnp.where(valid, sigma, 1.0))
    n_total = float(d_model * d_hidden)
    upd_rms = jnp.sqrt(jnp.where(valid, upd_sq, 0.0) * (1.0 / n_total))
    w_rms = jnp.sqrt(jnp.where(valid, w_sq, 0.0) * (1.0 / n_total))
    size = hyper_ref[1] * jnp.maximum(EPS_TWO, w_rms) / jnp.maximum(1.0, upd_rms / hyper_ref[2])
    scal[0:1, :] = row_mean
    scal[1:2, :] = size


def write_kernel(dims, grad, wv_in, wv_out, short_new, long_new, scal,
                 w_in_new, row_in_new, col_in_new, w_out_new, row_out_new, col_out_new,
                 stage_in, stage_out, pscale, qscale, sem_in, sem_out):
    layers, ms, ml, parts = dims
    sch, lch = ms // LANE, ml // LANE
    rows_in, rows_out = ms // parts, ml // parts

    for layer in range(layers):
        for kind, (out_s, out_l) in enumerate(((row_in_new, col_in_new), (col_out_new, row_out_new))):
            mat = 2 * layer + kind
            for j in range(sch):
                out_s[layer:layer + 1, j * LANE:(j + 1) * LANE] = short_new[mat, j:j + 1, :]
            for j in range(lch):
                out_l[layer:layer + 1, j * LANE:(j + 1) * LANE] = long_new[mat, j:j + 1, :]

    def out_copy(layer, kind, part):
        if kind == 0:
            return pltpu.make_async_copy(
                stage_in.at[part], w_in_new.at[layer, pl.ds(part * rows_in, rows_in)], sem_in.at[part])
        return pltpu.make_async_copy(
            stage_out.at[part], w_out_new.at[layer, pl.ds(part * rows_out, rows_out)], sem_out.at[part])

    def pick(row, mat):
        at = lax.broadcasted_iota(jnp.int32, (1, LANE), 1) == mat
        return jnp.sum(jnp.where(at, scal[row:row + 1, :], 0.0), axis=1, keepdims=True)

    def scales(mat, kind):
        row_mean = pick(0, mat)
        size = pick(1, mat)
        if kind == 0:
            p = size * lax.rsqrt(short_new[mat] / row_mean)
            qscale[...] = lax.rsqrt(long_new[mat])
        else:
            p = size * lax.rsqrt(short_new[mat])
            qscale[...] = lax.rsqrt(long_new[mat] / row_mean)
        for j in range(sch):
            pscale[j * LANE:(j + 1) * LANE, :] = jnp.broadcast_to(p[j:j + 1, :], (LANE, LANE)).T

    def one_layer(layer, carry):
        scales(2 * layer, 0)
        for part in range(parts):
            @pl.when(layer > 0)
            def _():
                out_copy(layer, 0, part).wait()

            r0 = part * rows_in

            def cols_in(j, inner):
                cols = pl.ds(pl.multiple_of(j * LANE, LANE), LANE)
                u = grad[2 * layer, r0:r0 + rows_in, cols] * pscale[r0:r0 + rows_in, :] * qscale[pl.ds(j, 1), :]
                stage_in[part, :, cols] = wv_in[layer, r0:r0 + rows_in, cols] - u
                return inner

            lax.fori_loop(0, lch, cols_in, 0)
            out_copy(layer, 0, part).start()

        scales(2 * layer + 1, 1)
        for part in range(parts):
            @pl.when(layer > 0)
            def _():
                out_copy(layer, 1, part).wait()

            j0 = part * (rows_out // LANE)

            def rows_loop(j, inner):
                cols = pl.ds(pl.multiple_of((j0 + j) * LANE, LANE), LANE)
                rows = pl.ds(pl.multiple_of(j * LANE, LANE), LANE)
                u = grad[2 * layer + 1, :, cols] * pscale[...] * qscale[pl.ds(j0 + j, 1), :]
                stage_out[part, rows, :] = wv_out[layer, cols, :] - u.T
                return inner

            lax.fori_loop(0, rows_out // LANE, rows_loop, 0)
            out_copy(layer, 1, part).start()
        return carry

    lax.fori_loop(0, layers, one_layer, 0)
    for kind in range(2):
        for part in range(parts):
            out_copy(layers - 1, kind, part).wait()


def solution(mesh):
    n_col = mesh.shape['col']
    n_row = mesh.shape['row']
    tile_in = P(None, 'row', 'col')
    tile_out = P(None, 'col', 'row')
    lane_row = P(None, None, 'row')
    lane_col = P(None, None, 'col')
    vec_row = P(None, 'row')
    vec_col = P(None, 'col')

    def local_step(hyper_params, w_in, x_in, dy_in, row_in, col_in, w_out, x_out, dy_out, row_out, col_out):
        layers, ms, ml = w_in.shape
        tokens = x_in.shape[1]
        mats = 2 * layers
        sch, lch = ms // LANE, ml // LANE
        n_dev = n_col * n_row
        d_model, d_hidden = ms * n_row, ml * n_col
        hbm_spec = pl.BlockSpec(memory_space=pltpu.HBM)
        vmem_spec = pl.BlockSpec(memory_space=pltpu.VMEM)
        dims = (n_col, n_row, layers, ms, ml, d_model, d_hidden)
        bf16 = jnp.bfloat16
        kept = pl.pallas_call(
            functools.partial(stats_kernel, dims),
            out_shape=(pltpu.VMEM((mats, ms, ml), F32), pltpu.VMEM((layers, ms, ml), F32),
                       pltpu.VMEM((layers, ml, ms), F32), pltpu.VMEM((mats, sch, LANE), F32),
                       pltpu.VMEM((mats, lch, LANE), F32), pltpu.VMEM((8, LANE), F32)),
            in_specs=[hbm_spec] * 11,
            out_specs=(vmem_spec,) * 6,
            scratch_shapes=[
                pltpu.VMEM((4, tokens, ms), bf16), pltpu.VMEM((4, tokens, ml), bf16),
                pltpu.VMEM((ms, tokens), bf16),
                pltpu.VMEM((layers, ms), F32), pltpu.VMEM((layers, ml), F32),
                pltpu.VMEM((layers, ms), F32), pltpu.VMEM((layers, ml), F32),
                pltpu.VMEM((mats, sch, LANE), F32), pltpu.VMEM((mats, lch, LANE), F32),
                pltpu.VMEM((mats, n_row, lch, LANE), F32), pltpu.VMEM((mats, n_col, sch, LANE), F32),
                pltpu.VMEM((n_dev, 1, LANE), F32),
                pltpu.VMEM((ms, LANE), F32), pltpu.VMEM((8, ml), F32), pltpu.VMEM((ms, LANE), F32),
                pltpu.VMEM((lch, LANE), F32), pltpu.VMEM((1, LANE), F32), pltpu.SMEM((3,), F32),
                pltpu.SemaphoreType.DMA((4, 2)), pltpu.SemaphoreType.DMA((layers, 2)),
                pltpu.SemaphoreType.DMA((5,)),
                pltpu.SemaphoreType.DMA((mats,)), pltpu.SemaphoreType.DMA((mats,)),
                pltpu.SemaphoreType.DMA((mats,)), pltpu.SemaphoreType.DMA((mats,)),
                pltpu.SemaphoreType.DMA, pltpu.SemaphoreType.DMA,
            ],
            compiler_params=pltpu.CompilerParams(
                collective_id=0, has_side_effects=True, vmem_limit_bytes=13 * 2 ** 20),
            name='stats',
        )(*(pltpu.with_memory_space_constraint(item, pltpu.HBM) for item in (
            hyper_params, w_in, x_in, dy_in, row_in, col_in, w_out, x_out, dy_out, row_out, col_out)))
        parts = 4
        return pl.pallas_call(
            functools.partial(write_kernel, (layers, ms, ml, parts)),
            out_shape=tuple(jax.ShapeDtypeStruct(item.shape, F32) for item in (
                w_in, row_in, col_in, w_out, row_out, col_out)),
            in_specs=[vmem_spec] * 6,
            out_specs=(hbm_spec, vmem_spec, vmem_spec, hbm_spec, vmem_spec, vmem_spec),
            scratch_shapes=[
                pltpu.VMEM((parts, ms // parts, ml), F32), pltpu.VMEM((parts, ml // parts, ms), F32),
                pltpu.VMEM((ms, LANE), F32), pltpu.VMEM((lch, LANE), F32),
                pltpu.SemaphoreType.DMA((parts,)), pltpu.SemaphoreType.DMA((parts,)),
            ],
            compiler_params=pltpu.CompilerParams(vmem_limit_bytes=13 * 2 ** 20),
            name='write',
        )(*kept)

    return jax.shard_map(local_step, mesh=mesh, in_specs=(P(), tile_in, lane_row, lane_col, vec_row, vec_col, tile_out, lane_col, lane_row, vec_col, vec_row), out_specs=(tile_in, vec_row, vec_col, tile_out, vec_col, vec_row), check_vma=False)
```

```python
import functools

import jax
import jax.numpy as jnp
from jax import lax
from jax.experimental import pallas as pl
from jax.experimental.pallas import tpu as pltpu
from jax.sharding import PartitionSpec as P

EPS_ONE = 1e-30
EPS_TWO = 1e-3
LANE = 128
CHUNK = 1280
UCOLS = 640
WCOLS = 512
MESH = pl.DeviceIdType.MESH
F32 = jnp.float32


def tree(items):
    while len(items) > 1:
        items = [items[k] + items[k + 1] if k + 1 < len(items) else items[k] for k in range(0, len(items), 2)]
    return items[0]


def stats_kernel(dims, hyper_hbm, w_in, x_in, dy_in, row_in, col_in, w_out, x_out, dy_out, row_out, col_out,
                 grad, wv_in, wv_out, short_new, long_new, scal,
                 act_s, act_l, lhs_t, old_s_in, old_l_in, old_s_out, old_l_out, short_old, long_old,
                 long_buf, short_buf, fin_buf, racc, cacc, rscale, linv, pack, hyper_ref,
                 act_sem, w_sem, old_sem, long_send, long_recv, short_send, short_recv, fin_send, fin_recv):
    n_col, n_row, layers, ms, ml, d_model, d_hidden = dims
    n_dev = n_col * n_row
    sch, lch = ms // LANE, ml // LANE
    my_col = lax.axis_index('col')
    my_row = lax.axis_index('row')

    def act_copies(layer, kind):
        slot = 2 * lax.rem(layer, 2) + kind
        src_s = (x_in, dy_out)[kind]
        src_l = (dy_in, x_out)[kind]
        return (pltpu.make_async_copy(src_s.at[layer], act_s.at[slot], act_sem.at[slot, 0]),
                pltpu.make_async_copy(src_l.at[layer], act_l.at[slot], act_sem.at[slot, 1]))

    def w_copy(layer, kind):
        src = (w_in, w_out)[kind]
        dst = (wv_in, wv_out)[kind]
        return pltpu.make_async_copy(src.at[layer], dst.at[layer], w_sem.at[layer, kind])

    old_copies = [pltpu.make_async_copy(src, dst, old_sem.at[idx]) for idx, (src, dst) in enumerate(
        ((row_in, old_s_in), (col_in, old_l_in), (col_out, old_s_out), (row_out, old_l_out), (hyper_hbm, hyper_ref)))]

    for layer in range(2):
        for kind in range(2):
            for copy in act_copies(layer, kind):
                copy.start()
    for copy in old_copies:
        copy.start()

    barrier = pltpu.get_barrier_semaphore()

    def peer_of(step):
        lin = lax.rem(my_col * n_row + my_row + step, n_dev)
        return (lin // n_row, lax.rem(lin, n_row))

    for step in range(1, n_dev):
        pl.semaphore_signal(barrier, inc=1, device_id=peer_of(step), device_id_type=MESH)

    pack[...] = jnp.zeros_like(pack)
    for copy in old_copies:
        copy.wait()
    beta_two = hyper_ref[0]
    for kind, (src_s, src_l) in enumerate(((old_s_in, old_l_in), (old_s_out, old_l_out))):
        for layer in range(layers):
            for j in range(sch):
                short_old[2 * layer + kind, j:j + 1, :] = src_s[layer:layer + 1, j * LANE:(j + 1) * LANE]
            for j in range(lch):
                long_old[2 * layer + kind, j:j + 1, :] = src_l[layer:layer + 1, j * LANE:(j + 1) * LANE]
    pl.semaphore_wait(barrier, n_dev - 1)

    def long_copy(mat, step):
        peer = lax.rem(my_row + step, n_row)
        return pltpu.make_async_remote_copy(
            src_ref=long_buf.at[mat, my_row], dst_ref=long_buf.at[mat, my_row],
            send_sem=long_send.at[mat], recv_sem=long_recv.at[mat],
            device_id=(my_col, peer), device_id_type=MESH)

    def short_copy(mat):
        return pltpu.make_async_remote_copy(
            src_ref=short_buf.at[mat, my_col], dst_ref=short_buf.at[mat, my_col],
            send_sem=short_send.at[mat], recv_sem=short_recv.at[mat],
            device_id=(n_col - 1 - my_col, my_row), device_id_type=MESH)

    def form_grad(layer, kind):
        mat = 2 * layer + kind
        slot = 2 * lax.rem(layer, 2) + kind
        for copy in act_copies(layer, kind):
            copy.wait()
        lhs_t[...] = act_s[slot].T
        racc[...] = jnp.zeros_like(racc)

        def chunk(c, carry):
            cols = pl.ds(pl.multiple_of(c * CHUNK, CHUNK), CHUNK)
            g = jnp.dot(lhs_t[...], act_l[slot, :, cols], preferred_element_type=F32)
            grad[mat, :, cols] = g
            sq = g * g
            racc[...] += tree([sq[:, j * LANE:(j + 1) * LANE] for j in range(CHUNK // LANE)])
            cacc[:, cols] = jnp.sum(sq.reshape(ms // 8, 8, CHUNK), axis=0)
            return carry

        lax.fori_loop(0, ml // CHUNK, chunk, 0)
        for j in range(lch):
            long_buf[mat, my_row, j:j + 1, :] = jnp.sum(cacc[:, j * LANE:(j + 1) * LANE], axis=0, keepdims=True)
        for j in range(sch):
            part = racc[j * LANE:(j + 1) * LANE, :].T
            short_buf[mat, my_col, j:j + 1, :] = jnp.sum(part, axis=0, keepdims=True)
        for step in range(1, n_row):
            long_copy(mat, step).start()
        short_copy(mat).start()

    def put(lane, value):
        at = lax.broadcasted_iota(jnp.int32, (1, LANE), 1) == lane
        pack[...] += jnp.where(at, value, 0.0)

    def total(value):
        return jnp.sum(jnp.sum(value, axis=1, keepdims=True), axis=0, keepdims=True)

    def update_sq(layer, kind):
        mat = 2 * layer + kind
        pltpu.make_async_copy(long_buf.at[mat, pl.ds(0, n_row - 1)], long_buf.at[mat, pl.ds(0, n_row - 1)],
                              long_recv.at[mat]).wait()
        short_copy(mat).wait_recv()
        lsum = long_buf[mat, 0]
        for dev in range(1, n_row):
            lsum = lsum + long_buf[mat, dev]
        ssum = short_buf[mat, 0]
        for dev in range(1, n_col):
            ssum = ssum + short_buf[mat, dev]
        lnew = beta_two * long_old[mat] + (1.0 - beta_two) * (lsum * (1.0 / d_model) + EPS_ONE)
        snew = beta_two * short_old[mat] + (1.0 - beta_two) * (ssum * (1.0 / d_hidden) + EPS_ONE)
        long_new[mat] = lnew
        short_new[mat] = snew
        if kind == 0:
            rho = total(snew)
            rs = lax.rsqrt(snew / (rho * (1.0 / ms)))
            linv[...] = 1.0 / lnew
        else:
            rho = total(lnew)
            rs = lax.rsqrt(snew)
            linv[...] = (rho * (1.0 / ml)) / lnew
        for j in range(sch):
            rscale[j * LANE:(j + 1) * LANE, :] = jnp.broadcast_to(rs[j:j + 1, :], (LANE, LANE)).T

        def chunk(c, acc):
            scale = rscale[...]
            for h in range(UCOLS // LANE):
                j = c * (UCOLS // LANE) + h
                u = grad[mat, :, pl.ds(pl.multiple_of(j * LANE, LANE), LANE)] * scale
                part = jnp.sum((u * u).reshape(ms // 8, 8, LANE), axis=0)
                acc = acc + part * linv[pl.ds(j, 1), :]
            return acc

        acc = lax.fori_loop(0, ml // UCOLS, chunk, jnp.zeros((8, LANE), F32))
        put(mat, total(acc))
        put(mat + 2 * layers, rho)

    def weight_sq(layer, kind):
        mat = 2 * layer + kind
        w_copy(layer, kind).wait()
        ref = (wv_in, wv_out)[kind]
        rows, cols = ref.shape[1:]
        block = max(8, 8 * 8 * 20 * LANE // cols)

        def chunk(t, acc):
            v = ref[layer, pl.ds(pl.multiple_of(t * block, 8), block), :]
            v = v * v
            part = tree([v[:, j * LANE:(j + 1) * LANE] for j in range(cols // LANE)])
            part = [part[8 * j:8 * j + 8] for j in range(block // 8)]
            return acc + tree(part)

        acc = lax.fori_loop(0, rows // block, chunk, jnp.zeros((8, LANE), F32))
        put(mat + 4 * layers, total(acc))

    def phase_one(layer, carry):
        for kind in range(2):
            form_grad(layer, kind)

            @pl.when(layer + 2 < layers)
            def _():
                for copy in act_copies(layer + 2, kind):
                    copy.start()

            w_copy(layer, kind).start()

        @pl.when(layer >= 2)
        def _():
            for kind in range(2):
                update_sq(layer - 2, kind)

        return carry

    lax.fori_loop(0, layers, phase_one, 0)

    def phase_two(layer, carry):
        @pl.when(layer >= layers - 2)
        def _():
            for kind in range(2):
                update_sq(layer, kind)

        for kind in range(2):
            weight_sq(layer, kind)
        return carry

    lax.fori_loop(0, layers, phase_two, 0)

    me = my_col * n_row + my_row
    fin_buf[me] = pack[...]

    def fin_copy(step):
        return pltpu.make_async_remote_copy(
            src_ref=fin_buf.at[me], dst_ref=fin_buf.at[me], send_sem=fin_send, recv_sem=fin_recv,
            device_id=peer_of(step), device_id_type=MESH)

    for step in range(1, n_dev):
        fin_copy(step).start()
    for mat in range(2 * layers):
        pltpu.make_async_copy(long_buf.at[mat, pl.ds(0, n_row - 1)], long_buf.at[mat, pl.ds(0, n_row - 1)],
                              long_send.at[mat]).wait()
        short_copy(mat).wait_send()
    others = fin_buf.at[pl.ds(0, n_dev - 1)]
    pltpu.make_async_copy(others, others, fin_send).wait()
    pltpu.make_async_copy(others, others, fin_recv).wait()

    lane = lax.broadcasted_iota(jnp.int32, (1, LANE), 1)
    is_in = lax.rem(lane, 2) == 0
    valid = lane < 2 * layers
    rho_sum = jnp.zeros((1, LANE), F32)
    w_sq = jnp.zeros((1, LANE), F32)
    for dev in range(n_dev):
        rho_sum = rho_sum + pltpu.roll(fin_buf[dev], LANE - 2 * layers, 1)
        w_sq = w_sq + pltpu.roll(fin_buf[dev], LANE - 4 * layers, 1)
    row_mean = rho_sum * jnp.where(is_in, 1.0 / (n_col * d_model), 1.0 / (n_row * d_hidden))
    row_mean = jnp.where(valid, row_mean, 1.0)
    upd_sq = jnp.zeros((1, LANE), F32)
    for dev in range(n_dev):
        sigma = pltpu.roll(fin_buf[dev], LANE - 2 * layers, 1) * jnp.where(is_in, 1.0 / ms, 1.0 / ml)
        upd_sq = upd_sq + fin_buf[dev] * (row_mean / jnp.where(valid, sigma, 1.0))
    n_total = float(d_model * d_hidden)
    upd_rms = jnp.sqrt(jnp.where(valid, upd_sq, 0.0) * (1.0 / n_total))
    w_rms = jnp.sqrt(jnp.where(valid, w_sq, 0.0) * (1.0 / n_total))
    size = hyper_ref[1] * jnp.maximum(EPS_TWO, w_rms) / jnp.maximum(1.0, upd_rms / hyper_ref[2])
    scal[0:1, :] = row_mean
    scal[1:2, :] = size


def write_kernel(dims, grad, wv_in, wv_out, short_new, long_new, scal,
                 w_in_new, row_in_new, col_in_new, w_out_new, row_out_new, col_out_new,
                 stage_in, stage_out, pscale, qscale, vec_s, vec_l, sem_in, sem_out, sem_vec):
    layers, ms, ml, parts = dims
    sch, lch = ms // LANE, ml // LANE
    rows_in, rows_out = ms // parts, ml // parts

    vec_copies = [pltpu.make_async_copy(src, dst, sem_vec.at[idx]) for idx, (src, dst) in enumerate(
        ((vec_s.at[0], row_in_new), (vec_l.at[0], col_in_new), (vec_s.at[1], col_out_new), (vec_l.at[1], row_out_new)))]

    def out_copy(layer, kind, part):
        if kind == 0:
            rows = pl.ds(pl.multiple_of(part * rows_in, rows_in), rows_in)
            return pltpu.make_async_copy(stage_in.at[part], w_in_new.at[layer, rows], sem_in.at[part])
        rows = pl.ds(pl.multiple_of(part * rows_out, rows_out), rows_out)
        return pltpu.make_async_copy(stage_out.at[part], w_out_new.at[layer, rows], sem_out.at[part])

    def pick(row, mat):
        at = lax.broadcasted_iota(jnp.int32, (1, LANE), 1) == mat
        return jnp.sum(jnp.where(at, scal[row:row + 1, :], 0.0), axis=1, keepdims=True)

    def scales(mat, kind):
        row_mean = pick(0, mat)
        size = pick(1, mat)
        if kind == 0:
            p = size * lax.rsqrt(short_new[mat] / row_mean)
            qscale[...] = lax.rsqrt(long_new[mat])
        else:
            p = size * lax.rsqrt(short_new[mat])
            qscale[...] = lax.rsqrt(long_new[mat] / row_mean)
        for j in range(sch):
            pscale[j * LANE:(j + 1) * LANE, :] = jnp.broadcast_to(p[j:j + 1, :], (LANE, LANE)).T

    def one_layer(layer, carry):
        scales(2 * layer, 0)

        def part_in(part, inner):
            @pl.when(layer > 0)
            def _():
                out_copy(layer, 0, part).wait()

            rows = pl.ds(pl.multiple_of(part * rows_in, rows_in), rows_in)

            def cols_in(c, inner2):
                p = pscale[rows, :]
                for h in range(WCOLS // LANE):
                    j = c * (WCOLS // LANE) + h
                    cols = pl.ds(pl.multiple_of(j * LANE, LANE), LANE)
                    u = grad[2 * layer, rows, cols] * p * qscale[pl.ds(j, 1), :]
                    stage_in[part, :, cols] = wv_in[layer, rows, cols] - u
                return inner2

            lax.fori_loop(0, ml // WCOLS, cols_in, 0)
            out_copy(layer, 0, part).start()
            return inner

        lax.fori_loop(0, parts, part_in, 0)
        scales(2 * layer + 1, 1)

        def part_out(part, inner):
            @pl.when(layer > 0)
            def _():
                out_copy(layer, 1, part).wait()

            p = pscale[...]
            for h in range(rows_out // LANE):
                j = part * (rows_out // LANE) + h
                cols = pl.ds(pl.multiple_of(j * LANE, LANE), LANE)
                u = grad[2 * layer + 1, :, cols] * p * qscale[pl.ds(j, 1), :]
                stage_out[part, h * LANE:(h + 1) * LANE, :] = wv_out[layer, cols, :] - u.T
            out_copy(layer, 1, part).start()
            return inner

        lax.fori_loop(0, parts, part_out, 0)

        @pl.when(layer == 0)
        def _():
            for each in range(layers):
                for kind in range(2):
                    mat = 2 * each + kind
                    for j in range(sch):
                        vec_s[kind, each:each + 1, j * LANE:(j + 1) * LANE] = short_new[mat, j:j + 1, :]
                    for j in range(lch):
                        vec_l[kind, each:each + 1, j * LANE:(j + 1) * LANE] = long_new[mat, j:j + 1, :]
            for copy in vec_copies:
                copy.start()

        return carry

    lax.fori_loop(0, layers, one_layer, 0)
    for kind in range(2):
        for part in range(parts):
            out_copy(layers - 1, kind, part).wait()
    for copy in vec_copies:
        copy.wait()


def solution(mesh):
    n_col = mesh.shape['col']
    n_row = mesh.shape['row']
    tile_in = P(None, 'row', 'col')
    tile_out = P(None, 'col', 'row')
    lane_row = P(None, None, 'row')
    lane_col = P(None, None, 'col')
    vec_row = P(None, 'row')
    vec_col = P(None, 'col')

    def local_step(hyper_params, w_in, x_in, dy_in, row_in, col_in, w_out, x_out, dy_out, row_out, col_out):
        layers, ms, ml = w_in.shape
        tokens = x_in.shape[1]
        mats = 2 * layers
        sch, lch = ms // LANE, ml // LANE
        n_dev = n_col * n_row
        d_model, d_hidden = ms * n_row, ml * n_col
        hbm_spec = pl.BlockSpec(memory_space=pltpu.HBM)
        vmem_spec = pl.BlockSpec(memory_space=pltpu.VMEM)
        dims = (n_col, n_row, layers, ms, ml, d_model, d_hidden)
        bf16 = jnp.bfloat16
        kept = pl.pallas_call(
            functools.partial(stats_kernel, dims),
            out_shape=(pltpu.VMEM((mats, ms, ml), F32), pltpu.VMEM((layers, ms, ml), F32),
                       pltpu.VMEM((layers, ml, ms), F32), pltpu.VMEM((mats, sch, LANE), F32),
                       pltpu.VMEM((mats, lch, LANE), F32), pltpu.VMEM((8, LANE), F32)),
            in_specs=[hbm_spec] * 11,
            out_specs=(vmem_spec,) * 6,
            scratch_shapes=[
                pltpu.VMEM((4, tokens, ms), bf16), pltpu.VMEM((4, tokens, ml), bf16),
                pltpu.VMEM((ms, tokens), bf16),
                pltpu.VMEM((layers, ms), F32), pltpu.VMEM((layers, ml), F32),
                pltpu.VMEM((layers, ms), F32), pltpu.VMEM((layers, ml), F32),
                pltpu.VMEM((mats, sch, LANE), F32), pltpu.VMEM((mats, lch, LANE), F32),
                pltpu.VMEM((mats, n_row, lch, LANE), F32), pltpu.VMEM((mats, n_col, sch, LANE), F32),
                pltpu.VMEM((n_dev, 1, LANE), F32),
                pltpu.VMEM((ms, LANE), F32), pltpu.VMEM((8, ml), F32), pltpu.VMEM((ms, LANE), F32),
                pltpu.VMEM((lch, LANE), F32), pltpu.VMEM((1, LANE), F32), pltpu.SMEM((3,), F32),
                pltpu.SemaphoreType.DMA((4, 2)), pltpu.SemaphoreType.DMA((layers, 2)),
                pltpu.SemaphoreType.DMA((5,)),
                pltpu.SemaphoreType.DMA((mats,)), pltpu.SemaphoreType.DMA((mats,)),
                pltpu.SemaphoreType.DMA((mats,)), pltpu.SemaphoreType.DMA((mats,)),
                pltpu.SemaphoreType.DMA, pltpu.SemaphoreType.DMA,
            ],
            compiler_params=pltpu.CompilerParams(
                collective_id=0, has_side_effects=True, vmem_limit_bytes=22 * 2 ** 20),
            name='stats',
        )(*(pltpu.with_memory_space_constraint(item, pltpu.HBM) for item in (
            hyper_params, w_in, x_in, dy_in, row_in, col_in, w_out, x_out, dy_out, row_out, col_out)))
        kept = tuple(pltpu.with_memory_space_constraint(item, pltpu.VMEM) for item in kept)
        parts = 4
        return pl.pallas_call(
            functools.partial(write_kernel, (layers, ms, ml, parts)),
            out_shape=tuple(jax.ShapeDtypeStruct(item.shape, F32) for item in (
                w_in, row_in, col_in, w_out, row_out, col_out)),
            in_specs=[vmem_spec] * 6,
            out_specs=(hbm_spec,) * 6,
            scratch_shapes=[
                pltpu.VMEM((parts, ms // parts, ml), F32), pltpu.VMEM((parts, ml // parts, ms), F32),
                pltpu.VMEM((ms, LANE), F32), pltpu.VMEM((lch, LANE), F32),
                pltpu.VMEM((2, layers, ms), F32), pltpu.VMEM((2, layers, ml), F32),
                pltpu.SemaphoreType.DMA((parts,)), pltpu.SemaphoreType.DMA((parts,)),
                pltpu.SemaphoreType.DMA((4,)),
            ],
            compiler_params=pltpu.CompilerParams(vmem_limit_bytes=22 * 2 ** 20),
            name='write',
        )(*kept)

    return jax.shard_map(local_step, mesh=mesh, in_specs=(P(), tile_in, lane_row, lane_col, vec_row, vec_col, tile_out, lane_col, lane_row, vec_col, vec_row), out_specs=(tile_in, vec_row, vec_col, tile_out, vec_col, vec_row), check_vma=False)
```

```python
import functools

import jax
import jax.numpy as jnp
from jax import lax
from jax.experimental import pallas as pl
from jax.experimental.pallas import tpu as pltpu
from jax.sharding import PartitionSpec as P

EPS_ONE = 1e-30
EPS_TWO = 1e-3
LANE = 128
CHUNK = 1280
MESH = pl.DeviceIdType.MESH
F32 = jnp.float32
VMEM_GRANT = 20 * 2 ** 20


def tree(items):
    while len(items) > 1:
        items = [items[k] + items[k + 1] if k + 1 < len(items) else items[k] for k in range(0, len(items), 2)]
    return items[0]


def total(value):
    return jnp.sum(jnp.sum(value, axis=1, keepdims=True), axis=0, keepdims=True)


def stats_kernel(dims, hyper_hbm, w_in, x_in, dy_in, row_in, col_in, w_out, x_out, dy_out, row_out, col_out,
                 grad_lo, grad_hi, wv_in, wv_out, short_new, long_new, short_scale, long_scale, step_size,
                 act_s, act_l, lhs_t, old_s_in, old_l_in, old_s_out, old_l_out, short_old, long_old,
                 long_buf, short_buf, upd_buf, wsq_buf, racc, cacc, linv, pack, wpack, hyper_ref,
                 act_sem, w_sem, old_sem, long_send, long_recv, short_send, short_recv, fin_send, fin_recv):
    n_col, n_row, layers, ms, ml, d_model, d_hidden = dims
    n_dev = n_col * n_row
    half = layers // 2
    sch, lch = ms // LANE, ml // LANE
    my_col = lax.axis_index('col')
    my_row = lax.axis_index('row')
    me = my_col * n_row + my_row

    def act_copies(layer, kind):
        slot = 2 * lax.rem(layer, 2) + kind
        src_s = (x_in, dy_out)[kind]
        src_l = (dy_in, x_out)[kind]
        return (pltpu.make_async_copy(src_s.at[layer], act_s.at[slot], act_sem.at[slot, 0]),
                pltpu.make_async_copy(src_l.at[layer], act_l.at[slot], act_sem.at[slot, 1]))

    def w_copy(layer, kind):
        src = (w_in, w_out)[kind]
        dst = (wv_in, wv_out)[kind]
        return pltpu.make_async_copy(src.at[layer], dst.at[layer], w_sem.at[layer, kind])

    old_copies = [pltpu.make_async_copy(src, dst, old_sem.at[idx]) for idx, (src, dst) in enumerate(
        ((row_in, old_s_in), (col_in, old_l_in), (col_out, old_s_out), (row_out, old_l_out), (hyper_hbm, hyper_ref)))]

    for layer in range(2):
        for kind in range(2):
            for copy in act_copies(layer, kind):
                copy.start()
    for copy in old_copies:
        copy.start()

    barrier = pltpu.get_barrier_semaphore()

    def peer_of(step):
        lin = lax.rem(me + step, n_dev)
        return (lin // n_row, lax.rem(lin, n_row))

    for step in range(1, n_dev):
        pl.semaphore_signal(barrier, inc=1, device_id=peer_of(step), device_id_type=MESH)

    pack[...] = jnp.zeros_like(pack)
    wpack[...] = jnp.zeros_like(wpack)

    def long_copy(mat, step):
        peer = lax.rem(my_row + step, n_row)
        return pltpu.make_async_remote_copy(
            src_ref=long_buf.at[mat, my_row], dst_ref=long_buf.at[mat, my_row],
            send_sem=long_send.at[mat], recv_sem=long_recv.at[mat],
            device_id=(my_col, peer), device_id_type=MESH)

    def short_copy(mat):
        return pltpu.make_async_remote_copy(
            src_ref=short_buf.at[mat, my_col], dst_ref=short_buf.at[mat, my_col],
            send_sem=short_send.at[mat], recv_sem=short_recv.at[mat],
            device_id=(n_col - 1 - my_col, my_row), device_id_type=MESH)

    def long_others(mat, sem):
        ref = long_buf.at[mat, pl.ds(0, n_row - 1)]
        return pltpu.make_async_copy(ref, ref, sem.at[mat])

    def fin_copy(buf, idx, step):
        return pltpu.make_async_remote_copy(
            src_ref=buf.at[me], dst_ref=buf.at[me], send_sem=fin_send.at[idx], recv_sem=fin_recv.at[idx],
            device_id=peer_of(step), device_id_type=MESH)

    def fin_others(buf, sem):
        ref = buf.at[pl.ds(0, n_dev - 1)]
        return pltpu.make_async_copy(ref, ref, sem)

    def put(where, lane, value):
        at = lax.broadcasted_iota(jnp.int32, (1, LANE), 1) == lane
        where[...] += jnp.where(at, value, 0.0)

    def dot_part(grad, base, mat, slot, c):
        cols = slice(c * CHUNK, (c + 1) * CHUNK)
        g = jnp.dot(lhs_t[...], act_l[slot, :, cols], preferred_element_type=F32)
        grad[mat - base, :, cols] = g
        sq = g * g
        part = tree([sq[:, j * LANE:(j + 1) * LANE] for j in range(CHUNK // LANE)])
        if c == 0:
            racc[...] = part
        else:
            racc[...] += part
        cacc[:, cols] = jnp.sum(sq.reshape(ms // 8, 8, CHUNK), axis=0)

    def upd_part(grad, base, mat, c):
        scale = short_scale[mat]
        acc = []
        for j in range(c * CHUNK // LANE, (c + 1) * CHUNK // LANE):
            u = grad[mat - base, :, j * LANE:(j + 1) * LANE] * scale
            acc.append(jnp.sum((u * u).reshape(ms // 8, 8, LANE), axis=0) * linv[j:j + 1, :])
        return tree(acc)

    def stats(layer, kind):
        mat = 2 * layer + kind
        long_others(mat, long_recv).wait()
        short_copy(mat).wait_recv()
        beta_two = hyper_ref[0]
        lsum = tree([long_buf[mat, dev] for dev in range(n_row)])
        ssum = tree([short_buf[mat, dev] for dev in range(n_col)])
        lnew = beta_two * long_old[mat] + (1.0 - beta_two) * (lsum * (1.0 / d_model) + EPS_ONE)
        snew = beta_two * short_old[mat] + (1.0 - beta_two) * (ssum * (1.0 / d_hidden) + EPS_ONE)
        long_new[mat] = lnew
        short_new[mat] = snew
        if kind == 0:
            rho = total(snew)
            rs = lax.rsqrt(snew / (rho * (1.0 / ms)))
            rl = lax.rsqrt(lnew)
        else:
            rho = total(lnew)
            rs = lax.rsqrt(snew)
            rl = lax.rsqrt(lnew / (rho * (1.0 / ml)))
        long_scale[mat] = rl
        linv[...] = rl * rl
        for j in range(sch):
            short_scale[mat, j * LANE:(j + 1) * LANE, :] = jnp.broadcast_to(rs[j:j + 1, :], (LANE, LANE)).T
        put(pack, mat + 2 * layers, rho)

    def send(mat):
        for j in range(lch):
            long_buf[mat, my_row, j:j + 1, :] = jnp.sum(cacc[:, j * LANE:(j + 1) * LANE], axis=0, keepdims=True)
        for j in range(sch):
            part = racc[j * LANE:(j + 1) * LANE, :].T
            short_buf[mat, my_col, j:j + 1, :] = jnp.sum(part, axis=0, keepdims=True)
        for step in range(1, n_row):
            long_copy(mat, step).start()
        short_copy(mat).start()

    def form_layer(layer, with_upd):
        for kind in range(2):
            mat = 2 * layer + kind
            slot = 2 * lax.rem(layer, 2) + kind
            for copy in act_copies(layer, kind):
                copy.wait()
            if with_upd:
                stats(layer - half, kind)
            lhs_t[...] = act_s[slot].T
            acc = []
            for c in range(ml // CHUNK):
                if with_upd:
                    acc.append(upd_part(grad_lo, 0, mat - 2 * half, c))
                dot_part(*((grad_hi, 2 * half) if with_upd else (grad_lo, 0)), mat, slot, c)
            if with_upd:
                put(pack, mat - 2 * half, total(tree(acc)))
            else:
                for copy in act_copies(layer + half, kind):
                    copy.start()
            w_copy(layer, kind).start()
            send(mat)

    def first_half(layer, carry):
        form_layer(layer, False)

        @pl.when(layer == 0)
        def _():
            for copy in old_copies:
                copy.wait()
            for kind, (src_s, src_l) in enumerate(((old_s_in, old_l_in), (old_s_out, old_l_out))):
                for each in range(layers):
                    for j in range(sch):
                        short_old[2 * each + kind, j:j + 1, :] = src_s[each:each + 1, j * LANE:(j + 1) * LANE]
                    for j in range(lch):
                        long_old[2 * each + kind, j:j + 1, :] = src_l[each:each + 1, j * LANE:(j + 1) * LANE]

        return carry

    def second_half(layer, carry):
        form_layer(layer, True)
        return carry

    def upd_tail(layer, carry):
        for kind in range(2):
            mat = 2 * layer + kind
            stats(layer, kind)
            put(pack, mat, total(tree([upd_part(grad_hi, 2 * half, mat, c) for c in range(ml // CHUNK)])))
        return carry

    pl.semaphore_wait(barrier, n_dev - 1)
    lax.fori_loop(0, half, first_half, 0)
    lax.fori_loop(half, layers, second_half, 0)
    lax.fori_loop(half, layers, upd_tail, 0)

    upd_buf[me] = pack[...]
    for step in range(1, n_dev):
        fin_copy(upd_buf, 0, step).start()

    def weight_sq(layer, kind):
        w_copy(layer, kind).wait()
        ref = (wv_in, wv_out)[kind]
        rows, cols = ref.shape[1:]
        block = max(8, 8 * 8 * 20 * LANE // cols)

        def chunk(t, acc):
            v = ref[layer, pl.ds(pl.multiple_of(t * block, 8), block), :]
            v = v * v
            part = tree([v[:, j * LANE:(j + 1) * LANE] for j in range(cols // LANE)])
            return acc + tree([part[8 * j:8 * j + 8] for j in range(block // 8)])

        acc = lax.fori_loop(0, rows // block, chunk, jnp.zeros((8, LANE), F32))
        put(wpack, 2 * layer + kind, total(acc))

    def weights(layer, carry):
        for kind in range(2):
            weight_sq(layer, kind)
        return carry

    lax.fori_loop(0, layers, weights, 0)
    wsq_buf[me] = wpack[...]
    for step in range(1, n_dev):
        fin_copy(wsq_buf, 1, step).start()

    for mat in range(2 * layers):
        long_others(mat, long_send).wait()
        short_copy(mat).wait_send()
    fin_others(upd_buf, fin_send.at[0]).wait()
    fin_others(upd_buf, fin_recv.at[0]).wait()
    lane = lax.broadcasted_iota(jnp.int32, (1, LANE), 1)
    is_in = lax.rem(lane, 2) == 0
    valid = lane < 2 * layers
    shift = LANE - 2 * layers
    rho_sum = pltpu.roll(tree([upd_buf[dev] for dev in range(n_dev)]), shift, 1)
    row_mean = rho_sum * jnp.where(is_in, 1.0 / (n_col * d_model), 1.0 / (n_row * d_hidden))
    row_mean = jnp.where(valid, row_mean, 1.0)
    per_block = jnp.where(is_in, 1.0 / ms, 1.0 / ml)

    def ratio(rho):
        return row_mean / jnp.where(valid, pltpu.roll(rho, shift, 1) * per_block, 1.0)

    upd_sq = tree([upd_buf[dev] * ratio(upd_buf[dev]) for dev in range(n_dev)])
    n_total = float(d_model * d_hidden)
    upd_rms = jnp.sqrt(jnp.where(valid, upd_sq, 0.0) * (1.0 / n_total))
    before_w = hyper_ref[1] * jnp.sqrt(ratio(pack[...])) / jnp.maximum(1.0, upd_rms / hyper_ref[2])

    fin_others(wsq_buf, fin_send.at[1]).wait()
    fin_others(wsq_buf, fin_recv.at[1]).wait()
    w_sq = tree([wsq_buf[dev] for dev in range(n_dev)])
    w_rms = jnp.sqrt(w_sq * (1.0 / n_total))
    size = before_w * jnp.maximum(EPS_TWO, w_rms)
    step_size[...] = jnp.broadcast_to(size, (LANE, LANE)).T[:2 * layers, :]


def write_kernel(dims, grad_lo, grad_hi, wv_in, wv_out, short_new, long_new, short_scale, long_scale, step_size,
                 w_in_new, row_in_new, col_in_new, w_out_new, row_out_new, col_out_new,
                 stage_in, stage_out, vec_s, vec_l, sem_in, sem_out, sem_vec):
    layers, ms, ml, parts = dims
    half = layers // 2
    sch, lch = ms // LANE, ml // LANE
    rows_in, rows_out = ms // parts, ml // parts

    vec_copies = [pltpu.make_async_copy(src, dst, sem_vec.at[idx]) for idx, (src, dst) in enumerate(
        ((vec_s.at[0], row_in_new), (vec_l.at[0], col_in_new), (vec_s.at[1], col_out_new), (vec_l.at[1], row_out_new)))]

    def out_copy(layer, kind, part):
        if kind == 0:
            rows = pl.ds(pl.multiple_of(part * rows_in, rows_in), rows_in)
            return pltpu.make_async_copy(stage_in.at[part], w_in_new.at[layer, rows], sem_in.at[part])
        rows = pl.ds(pl.multiple_of(part * rows_out, rows_out), rows_out)
        return pltpu.make_async_copy(stage_out.at[part], w_out_new.at[layer, rows], sem_out.at[part])

    def one_part(layer, grad, mat, part):
        @pl.when(layer > 0)
        def _():
            for kind in range(2):
                out_copy(layer, kind, part).wait()

        rows = pl.ds(pl.multiple_of(part * rows_in, rows_in), rows_in)
        p_out = short_scale[2 * layer + 1] * step_size[pl.ds(2 * layer + 1, 1), :]
        p_in = short_scale[2 * layer, rows, :] * step_size[pl.ds(2 * layer, 1), :]
        per_row = rows_out // LANE
        for h in range(per_row):
            j = part * per_row + h
            cols = pl.ds(pl.multiple_of(j * LANE, LANE), LANE)
            u = grad[mat + 1, :, cols] * p_out * long_scale[2 * layer + 1, pl.ds(j, 1), :]
            stage_out[part, h * LANE:(h + 1) * LANE, :] = wv_out[layer, cols, :] - u.T
            for j in range(h * (lch // per_row), (h + 1) * (lch // per_row)):
                cols = slice(j * LANE, (j + 1) * LANE)
                u = grad[mat, rows, cols] * p_in * long_scale[2 * layer, j:j + 1, :]
                stage_in[part, :, cols] = wv_in[layer, rows, cols] - u
        for kind in range(2):
            out_copy(layer, kind, part).start()

    def loop(base, grad):
        def one(t, carry):
            layer = base + t // parts
            one_part(layer, grad, 2 * (t // parts), lax.rem(t, parts))
            return carry

        lax.fori_loop(0, half * parts, one, 0)

    loop(0, grad_lo)
    for each in range(layers):
        for kind in range(2):
            mat = 2 * each + kind
            for j in range(sch):
                vec_s[kind, each:each + 1, j * LANE:(j + 1) * LANE] = short_new[mat, j:j + 1, :]
            for j in range(lch):
                vec_l[kind, each:each + 1, j * LANE:(j + 1) * LANE] = long_new[mat, j:j + 1, :]
    for copy in vec_copies:
        copy.start()
    loop(half, grad_hi)
    for kind in range(2):
        for part in range(parts):
            out_copy(layers - 1, kind, part).wait()
    for copy in vec_copies:
        copy.wait()


def solution(mesh):
    n_col = mesh.shape['col']
    n_row = mesh.shape['row']
    tile_in = P(None, 'row', 'col')
    tile_out = P(None, 'col', 'row')
    lane_row = P(None, None, 'row')
    lane_col = P(None, None, 'col')
    vec_row = P(None, 'row')
    vec_col = P(None, 'col')

    def local_step(hyper_params, w_in, x_in, dy_in, row_in, col_in, w_out, x_out, dy_out, row_out, col_out):
        layers, ms, ml = w_in.shape
        tokens = x_in.shape[1]
        mats = 2 * layers
        sch, lch = ms // LANE, ml // LANE
        n_dev = n_col * n_row
        d_model, d_hidden = ms * n_row, ml * n_col
        hbm_spec = pl.BlockSpec(memory_space=pltpu.HBM)
        vmem_spec = pl.BlockSpec(memory_space=pltpu.VMEM)
        dims = (n_col, n_row, layers, ms, ml, d_model, d_hidden)
        bf16 = jnp.bfloat16
        dma = pltpu.SemaphoreType.DMA
        kept = pl.pallas_call(
            functools.partial(stats_kernel, dims),
            out_shape=(pltpu.VMEM((layers, ms, ml), F32), pltpu.VMEM((layers, ms, ml), F32),
                       pltpu.VMEM((layers, ms, ml), F32), pltpu.VMEM((layers, ml, ms), F32),
                       pltpu.VMEM((mats, sch, LANE), F32), pltpu.VMEM((mats, lch, LANE), F32),
                       pltpu.VMEM((mats, ms, LANE), F32), pltpu.VMEM((mats, lch, LANE), F32),
                       pltpu.VMEM((mats, LANE), F32)),
            in_specs=[hbm_spec] * 11,
            out_specs=(vmem_spec,) * 9,
            scratch_shapes=[
                pltpu.VMEM((4, tokens, ms), bf16), pltpu.VMEM((4, tokens, ml), bf16),
                pltpu.VMEM((ms, tokens), bf16),
                pltpu.VMEM((layers, ms), F32), pltpu.VMEM((layers, ml), F32),
                pltpu.VMEM((layers, ms), F32), pltpu.VMEM((layers, ml), F32),
                pltpu.VMEM((mats, sch, LANE), F32), pltpu.VMEM((mats, lch, LANE), F32),
                pltpu.VMEM((mats, n_row, lch, LANE), F32), pltpu.VMEM((mats, n_col, sch, LANE), F32),
                pltpu.VMEM((n_dev, 1, LANE), F32), pltpu.VMEM((n_dev, 1, LANE), F32),
                pltpu.VMEM((ms, LANE), F32), pltpu.VMEM((8, ml), F32),
                pltpu.VMEM((lch, LANE), F32), pltpu.VMEM((1, LANE), F32), pltpu.VMEM((1, LANE), F32),
                pltpu.SMEM((3,), F32),
                dma((4, 2)), dma((layers, 2)), dma((5,)),
                dma((mats,)), dma((mats,)), dma((mats,)), dma((mats,)), dma((2,)), dma((2,)),
            ],
            compiler_params=pltpu.CompilerParams(
                collective_id=0, has_side_effects=True, vmem_limit_bytes=VMEM_GRANT),
            name='stats',
        )(*(pltpu.with_memory_space_constraint(item, pltpu.HBM) for item in (
            hyper_params, w_in, x_in, dy_in, row_in, col_in, w_out, x_out, dy_out, row_out, col_out)))
        kept = tuple(pltpu.with_memory_space_constraint(item, pltpu.VMEM) for item in kept)
        parts = 4
        return pl.pallas_call(
            functools.partial(write_kernel, (layers, ms, ml, parts)),
            out_shape=tuple(jax.ShapeDtypeStruct(item.shape, F32) for item in (
                w_in, row_in, col_in, w_out, row_out, col_out)),
            in_specs=[vmem_spec] * 9,
            out_specs=(hbm_spec,) * 6,
            scratch_shapes=[
                pltpu.VMEM((parts, ms // parts, ml), F32), pltpu.VMEM((parts, ml // parts, ms), F32),
                pltpu.VMEM((2, layers, ms), F32), pltpu.VMEM((2, layers, ml), F32),
                dma((parts,)), dma((parts,)), dma((4,)),
            ],
            compiler_params=pltpu.CompilerParams(vmem_limit_bytes=VMEM_GRANT),
            name='write',
        )(*kept)

    return jax.shard_map(local_step, mesh=mesh, in_specs=(P(), tile_in, lane_row, lane_col, vec_row, vec_col, tile_out, lane_col, lane_row, vec_col, vec_row), out_specs=(tile_in, vec_row, vec_col, tile_out, vec_col, vec_row), check_vma=False)
```

```python
import functools

import jax
import jax.numpy as jnp
from jax import lax
from jax.experimental import pallas as pl
from jax.experimental.pallas import tpu as pltpu
from jax.sharding import PartitionSpec as P

EPS_ONE = 1e-30
EPS_TWO = 1e-3
LANE = 128
CHUNK = 1280
WSTEPS = 8
MESH = pl.DeviceIdType.MESH
F32 = jnp.float32
VMEM_GRANT = 20 * 2 ** 20


def tree(items):
    while len(items) > 1:
        items = [items[k] + items[k + 1] if k + 1 < len(items) else items[k] for k in range(0, len(items), 2)]
    return items[0]


def total(value):
    return jnp.sum(jnp.sum(value, axis=1, keepdims=True), axis=0, keepdims=True)


def stats_kernel(dims, hyper_hbm, w_in, x_in, dy_in, row_in, col_in, w_out, x_out, dy_out, row_out, col_out,
                 grad_lo, grad_hi, wv_in, wv_out, short_new, long_new, short_scale, long_scale, step_size,
                 act_s, act_l, lhs_t, old_s_in, old_l_in, old_s_out, old_l_out, short_old, long_old,
                 long_buf, short_buf, upd_buf, wsq_buf, racc, cacc, linv, pack, wpack, hyper_ref,
                 act_sem, w_sem, old_sem, long_send, long_recv, short_send, short_recv, fin_send, fin_recv):
    n_col, n_row, layers, ms, ml, d_model, d_hidden = dims
    n_dev = n_col * n_row
    half = layers // 2
    sch, lch = ms // LANE, ml // LANE
    my_col = lax.axis_index('col')
    my_row = lax.axis_index('row')
    me = my_col * n_row + my_row

    def act_copies(layer, kind):
        slot = 2 * lax.rem(layer, 2) + kind
        src_s = (x_in, dy_out)[kind]
        src_l = (dy_in, x_out)[kind]
        return (pltpu.make_async_copy(src_s.at[layer], act_s.at[slot], act_sem.at[slot, 0]),
                pltpu.make_async_copy(src_l.at[layer], act_l.at[slot], act_sem.at[slot, 1]))

    def w_copy(layer, kind):
        src = (w_in, w_out)[kind]
        dst = (wv_in, wv_out)[kind]
        return pltpu.make_async_copy(src.at[layer], dst.at[layer], w_sem.at[layer, kind])

    old_copies = [pltpu.make_async_copy(src, dst, old_sem.at[idx]) for idx, (src, dst) in enumerate(
        ((row_in, old_s_in), (col_in, old_l_in), (col_out, old_s_out), (row_out, old_l_out), (hyper_hbm, hyper_ref)))]

    for layer in range(2):
        for kind in range(2):
            for copy in act_copies(layer, kind):
                copy.start()
    for copy in old_copies:
        copy.start()
    for layer in range(layers):
        for kind in range(2):
            w_copy(layer, kind).start(priority=1)

    barrier = pltpu.get_barrier_semaphore()

    def peer_of(step):
        lin = lax.rem(me + step, n_dev)
        return (lin // n_row, lax.rem(lin, n_row))

    for step in range(1, n_dev):
        pl.semaphore_signal(barrier, inc=1, device_id=peer_of(step), device_id_type=MESH)

    pack[...] = jnp.zeros_like(pack)
    wpack[...] = jnp.zeros_like(wpack)

    def long_copy(mat, step):
        peer = lax.rem(my_row + step, n_row)
        return pltpu.make_async_remote_copy(
            src_ref=long_buf.at[mat, my_row], dst_ref=long_buf.at[mat, my_row],
            send_sem=long_send.at[mat], recv_sem=long_recv.at[mat],
            device_id=(my_col, peer), device_id_type=MESH)

    def short_copy(mat):
        return pltpu.make_async_remote_copy(
            src_ref=short_buf.at[mat, my_col], dst_ref=short_buf.at[mat, my_col],
            send_sem=short_send.at[mat], recv_sem=short_recv.at[mat],
            device_id=(n_col - 1 - my_col, my_row), device_id_type=MESH)

    def long_others(mat, sem):
        ref = long_buf.at[mat, pl.ds(0, n_row - 1)]
        return pltpu.make_async_copy(ref, ref, sem.at[mat])

    def fin_copy(buf, idx, step):
        return pltpu.make_async_remote_copy(
            src_ref=buf.at[me], dst_ref=buf.at[me], send_sem=fin_send.at[idx], recv_sem=fin_recv.at[idx],
            device_id=peer_of(step), device_id_type=MESH)

    def fin_others(buf, sem):
        ref = buf.at[pl.ds(0, n_dev - 1)]
        return pltpu.make_async_copy(ref, ref, sem)

    def put(where, lane, value):
        at = lax.broadcasted_iota(jnp.int32, (1, LANE), 1) == lane
        where[...] += jnp.where(at, value, 0.0)

    def dot_part(grad, base, mat, slot, c):
        cols = slice(c * CHUNK, (c + 1) * CHUNK)
        g = jnp.dot(lhs_t[...], act_l[slot, :, cols], preferred_element_type=F32)
        grad[mat - base, :, cols] = g
        sq = g * g
        part = tree([sq[:, j * LANE:(j + 1) * LANE] for j in range(CHUNK // LANE)])
        if c == 0:
            racc[...] = part
        else:
            racc[...] += part
        cacc[:, cols] = jnp.sum(sq.reshape(ms // 8, 8, CHUNK), axis=0)

    def upd_part(grad, base, mat, c):
        cols = slice(c * CHUNK, (c + 1) * CHUNK)
        acc = jnp.zeros((8, CHUNK), F32)
        for r in range(0, ms, 8):
            u = grad[mat - base, r:r + 8, cols] * jnp.tile(short_scale[mat, r:r + 8, :], (1, CHUNK // LANE))
            acc = acc + u * u
        first = c * CHUNK // LANE
        return tree([acc[:, j * LANE:(j + 1) * LANE] * linv[first + j:first + j + 1, :] for j in range(CHUNK // LANE)])

    def stats(layer, kind):
        mat = 2 * layer + kind
        long_others(mat, long_recv).wait()
        short_copy(mat).wait_recv()
        beta_two = hyper_ref[0]
        lsum = tree([long_buf[mat, dev] for dev in range(n_row)])
        ssum = tree([short_buf[mat, dev] for dev in range(n_col)])
        lnew = beta_two * long_old[mat] + (1.0 - beta_two) * (lsum * (1.0 / d_model) + EPS_ONE)
        snew = beta_two * short_old[mat] + (1.0 - beta_two) * (ssum * (1.0 / d_hidden) + EPS_ONE)
        long_new[mat] = lnew
        short_new[mat] = snew
        if kind == 0:
            rho = total(snew)
            rs = lax.rsqrt(snew / (rho * (1.0 / ms)))
            rl = lax.rsqrt(lnew)
        else:
            rho = total(lnew)
            rs = lax.rsqrt(snew)
            rl = lax.rsqrt(lnew / (rho * (1.0 / ml)))
        long_scale[mat] = rl
        linv[...] = rl * rl
        for j in range(sch):
            short_scale[mat, j * LANE:(j + 1) * LANE, :] = jnp.broadcast_to(rs[j:j + 1, :], (LANE, LANE)).T
        put(pack, mat + 2 * layers, rho)

    def send(mat):
        for j in range(lch):
            long_buf[mat, my_row, j:j + 1, :] = jnp.sum(cacc[:, j * LANE:(j + 1) * LANE], axis=0, keepdims=True)
        for j in range(sch):
            part = racc[j * LANE:(j + 1) * LANE, :].T
            short_buf[mat, my_col, j:j + 1, :] = jnp.sum(part, axis=0, keepdims=True)
        for step in range(1, n_row):
            long_copy(mat, step).start()
        short_copy(mat).start()

    def form_layer(layer, with_upd):
        for kind in range(2):
            mat = 2 * layer + kind
            slot = 2 * lax.rem(layer, 2) + kind
            for copy in act_copies(layer, kind):
                copy.wait()
            if with_upd:
                stats(layer - half, kind)
            lhs_t[...] = act_s[slot].T
            acc = []
            for c in range(ml // CHUNK):
                if with_upd:
                    acc.append(upd_part(grad_lo, 0, mat - 2 * half, c))
                dot_part(*((grad_hi, 2 * half) if with_upd else (grad_lo, 0)), mat, slot, c)
            if with_upd:
                put(pack, mat - 2 * half, total(tree(acc)))
            else:
                for copy in act_copies(layer + half, kind):
                    copy.start()
            if kind == 0 and not with_upd:
                @pl.when(layer == 0)
                def _():
                    pl.semaphore_wait(barrier, n_dev - 1)

            send(mat)

    def first_half(layer, carry):
        form_layer(layer, False)

        @pl.when(layer == 0)
        def _():
            for copy in old_copies:
                copy.wait()
            for kind, (src_s, src_l) in enumerate(((old_s_in, old_l_in), (old_s_out, old_l_out))):
                for each in range(layers):
                    for j in range(sch):
                        short_old[2 * each + kind, j:j + 1, :] = src_s[each:each + 1, j * LANE:(j + 1) * LANE]
                    for j in range(lch):
                        long_old[2 * each + kind, j:j + 1, :] = src_l[each:each + 1, j * LANE:(j + 1) * LANE]

        return carry

    def second_half(layer, carry):
        form_layer(layer, True)
        return carry

    def upd_tail(layer, carry):
        for kind in range(2):
            mat = 2 * layer + kind
            stats(layer, kind)
            put(pack, mat, total(tree([upd_part(grad_hi, 2 * half, mat, c) for c in range(ml // CHUNK)])))
        return carry

    lax.fori_loop(0, half, first_half, 0)
    lax.fori_loop(half, layers, second_half, 0)
    def weight_sq(layer, kind):
        w_copy(layer, kind).wait()
        ref = (wv_in, wv_out)[kind]
        rows, cols = ref.shape[1:]
        slab = max(8, 80 * LANE // cols // 8 * 8)
        width = min(cols, 10 * LANE)
        trip = WSTEPS * slab

        def chunk(t, acc):
            for step in range(WSTEPS):
                at = pl.ds(pl.multiple_of(t * trip + step * slab, 8), slab)
                for c in range(0, cols, width):
                    v = ref[layer, at, c:c + width]
                    acc = acc + v * v
            return acc

        acc = lax.fori_loop(0, rows // trip, chunk, jnp.zeros((slab, width), F32))
        acc = tree([acc[:, j * LANE:(j + 1) * LANE] for j in range(width // LANE)])
        put(wpack, 2 * layer + kind, total(tree([acc[j:j + 8] for j in range(0, slab, 8)])))

    def weights(layer, carry):
        for kind in range(2):
            weight_sq(layer, kind)
        return carry

    lax.fori_loop(0, layers - 1, weights, 0)
    lax.fori_loop(half, layers, upd_tail, 0)
    upd_buf[me] = pack[...]
    for step in range(1, n_dev):
        fin_copy(upd_buf, 0, step).start()

    lax.fori_loop(layers - 1, layers, weights, 0)
    wsq_buf[me] = wpack[...]
    for step in range(1, n_dev):
        fin_copy(wsq_buf, 1, step).start()

    for mat in range(2 * layers):
        long_others(mat, long_send).wait()
        short_copy(mat).wait_send()
    fin_others(upd_buf, fin_send.at[0]).wait()
    fin_others(upd_buf, fin_recv.at[0]).wait()
    lane = lax.broadcasted_iota(jnp.int32, (1, LANE), 1)
    is_in = lax.rem(lane, 2) == 0
    valid = lane < 2 * layers
    shift = LANE - 2 * layers
    rho_sum = pltpu.roll(tree([upd_buf[dev] for dev in range(n_dev)]), shift, 1)
    row_mean = rho_sum * jnp.where(is_in, 1.0 / (n_col * d_model), 1.0 / (n_row * d_hidden))
    row_mean = jnp.where(valid, row_mean, 1.0)
    per_block = jnp.where(is_in, 1.0 / ms, 1.0 / ml)

    def ratio(rho):
        return row_mean / jnp.where(valid, pltpu.roll(rho, shift, 1) * per_block, 1.0)

    upd_sq = tree([upd_buf[dev] * ratio(upd_buf[dev]) for dev in range(n_dev)])
    n_total = float(d_model * d_hidden)
    upd_rms = jnp.sqrt(jnp.where(valid, upd_sq, 0.0) * (1.0 / n_total))
    before_w = hyper_ref[1] * jnp.sqrt(ratio(pack[...])) / jnp.maximum(1.0, upd_rms / hyper_ref[2])

    fin_others(wsq_buf, fin_send.at[1]).wait()
    fin_others(wsq_buf, fin_recv.at[1]).wait()
    w_sq = tree([wsq_buf[dev] for dev in range(n_dev)])
    w_rms = jnp.sqrt(w_sq * (1.0 / n_total))
    size = before_w * jnp.maximum(EPS_TWO, w_rms)
    step_size[...] = jnp.broadcast_to(size, (LANE, LANE)).T[:2 * layers, :]


def write_kernel(dims, grad_lo, grad_hi, wv_in, wv_out, short_new, long_new, short_scale, long_scale, step_size,
                 w_in_new, row_in_new, col_in_new, w_out_new, row_out_new, col_out_new,
                 stage_in, stage_out, vec_s, vec_l, sem_in, sem_out, sem_vec):
    layers, ms, ml, parts = dims
    half = layers // 2
    sch, lch = ms // LANE, ml // LANE
    rows_in, rows_out = ms // parts, ml // parts

    vec_copies = [pltpu.make_async_copy(src, dst, sem_vec.at[idx]) for idx, (src, dst) in enumerate(
        ((vec_s.at[0], row_in_new), (vec_l.at[0], col_in_new), (vec_s.at[1], col_out_new), (vec_l.at[1], row_out_new)))]

    def out_copy(layer, kind, part):
        if kind == 0:
            rows = pl.ds(pl.multiple_of(part * rows_in, rows_in), rows_in)
            return pltpu.make_async_copy(stage_in.at[part], w_in_new.at[layer, rows], sem_in.at[part])
        rows = pl.ds(pl.multiple_of(part * rows_out, rows_out), rows_out)
        return pltpu.make_async_copy(stage_out.at[part], w_out_new.at[layer, rows], sem_out.at[part])

    def one_part(layer, grad, mat, part):
        @pl.when(layer > 0)
        def _():
            for kind in range(2):
                out_copy(layer, kind, part).wait()

        rows = pl.ds(pl.multiple_of(part * rows_in, rows_in), rows_in)
        p_out = short_scale[2 * layer + 1] * step_size[pl.ds(2 * layer + 1, 1), :]
        p_in = short_scale[2 * layer, rows, :] * step_size[pl.ds(2 * layer, 1), :]
        per_row = rows_out // LANE
        for h in range(per_row):
            j = part * per_row + h
            cols = pl.ds(pl.multiple_of(j * LANE, LANE), LANE)
            u = grad[mat + 1, :, cols] * p_out * long_scale[2 * layer + 1, pl.ds(j, 1), :]
            stage_out[part, h * LANE:(h + 1) * LANE, :] = wv_out[layer, cols, :] - u.T
            for j in range(h * (lch // per_row), (h + 1) * (lch // per_row)):
                cols = slice(j * LANE, (j + 1) * LANE)
                u = grad[mat, rows, cols] * p_in * long_scale[2 * layer, j:j + 1, :]
                stage_in[part, :, cols] = wv_in[layer, rows, cols] - u
        for kind in range(2):
            out_copy(layer, kind, part).start()

    def loop(base, grad):
        def one(t, carry):
            layer = base + t // parts
            one_part(layer, grad, 2 * (t // parts), lax.rem(t, parts))
            return carry

        lax.fori_loop(0, half * parts, one, 0)

    loop(0, grad_lo)
    for each in range(layers):
        for kind in range(2):
            mat = 2 * each + kind
            for j in range(sch):
                vec_s[kind, each:each + 1, j * LANE:(j + 1) * LANE] = short_new[mat, j:j + 1, :]
            for j in range(lch):
                vec_l[kind, each:each + 1, j * LANE:(j + 1) * LANE] = long_new[mat, j:j + 1, :]
    for copy in vec_copies:
        copy.start()
    loop(half, grad_hi)
    for kind in range(2):
        for part in range(parts):
            out_copy(layers - 1, kind, part).wait()
    for copy in vec_copies:
        copy.wait()


def solution(mesh):
    n_col = mesh.shape['col']
    n_row = mesh.shape['row']
    tile_in = P(None, 'row', 'col')
    tile_out = P(None, 'col', 'row')
    lane_row = P(None, None, 'row')
    lane_col = P(None, None, 'col')
    vec_row = P(None, 'row')
    vec_col = P(None, 'col')

    def local_step(hyper_params, w_in, x_in, dy_in, row_in, col_in, w_out, x_out, dy_out, row_out, col_out):
        layers, ms, ml = w_in.shape
        tokens = x_in.shape[1]
        mats = 2 * layers
        sch, lch = ms // LANE, ml // LANE
        n_dev = n_col * n_row
        d_model, d_hidden = ms * n_row, ml * n_col
        hbm_spec = pl.BlockSpec(memory_space=pltpu.HBM)
        vmem_spec = pl.BlockSpec(memory_space=pltpu.VMEM)
        dims = (n_col, n_row, layers, ms, ml, d_model, d_hidden)
        bf16 = jnp.bfloat16
        dma = pltpu.SemaphoreType.DMA
        kept = pl.pallas_call(
            functools.partial(stats_kernel, dims),
            out_shape=(pltpu.VMEM((layers, ms, ml), F32), pltpu.VMEM((layers, ms, ml), F32),
                       pltpu.VMEM((layers, ms, ml), F32), pltpu.VMEM((layers, ml, ms), F32),
                       pltpu.VMEM((mats, sch, LANE), F32), pltpu.VMEM((mats, lch, LANE), F32),
                       pltpu.VMEM((mats, ms, LANE), F32), pltpu.VMEM((mats, lch, LANE), F32),
                       pltpu.VMEM((mats, LANE), F32)),
            in_specs=[hbm_spec] * 11,
            out_specs=(vmem_spec,) * 9,
            scratch_shapes=[
                pltpu.VMEM((4, tokens, ms), bf16), pltpu.VMEM((4, tokens, ml), bf16),
                pltpu.VMEM((ms, tokens), bf16),
                pltpu.VMEM((layers, ms), F32), pltpu.VMEM((layers, ml), F32),
                pltpu.VMEM((layers, ms), F32), pltpu.VMEM((layers, ml), F32),
                pltpu.VMEM((mats, sch, LANE), F32), pltpu.VMEM((mats, lch, LANE), F32),
                pltpu.VMEM((mats, n_row, lch, LANE), F32), pltpu.VMEM((mats, n_col, sch, LANE), F32),
                pltpu.VMEM((n_dev, 1, LANE), F32), pltpu.VMEM((n_dev, 1, LANE), F32),
                pltpu.VMEM((ms, LANE), F32), pltpu.VMEM((8, ml), F32),
                pltpu.VMEM((lch, LANE), F32), pltpu.VMEM((1, LANE), F32), pltpu.VMEM((1, LANE), F32),
                pltpu.SMEM((3,), F32),
                dma((4, 2)), dma((layers, 2)), dma((5,)),
                dma((mats,)), dma((mats,)), dma((mats,)), dma((mats,)), dma((2,)), dma((2,)),
            ],
            compiler_params=pltpu.CompilerParams(
                collective_id=0, has_side_effects=True, vmem_limit_bytes=VMEM_GRANT),
            name='stats',
        )(*(pltpu.with_memory_space_constraint(item, pltpu.HBM) for item in (
            hyper_params, w_in, x_in, dy_in, row_in, col_in, w_out, x_out, dy_out, row_out, col_out)))
        kept = tuple(pltpu.with_memory_space_constraint(item, pltpu.VMEM) for item in kept)
        parts = 4
        return pl.pallas_call(
            functools.partial(write_kernel, (layers, ms, ml, parts)),
            out_shape=tuple(jax.ShapeDtypeStruct(item.shape, F32) for item in (
                w_in, row_in, col_in, w_out, row_out, col_out)),
            in_specs=[vmem_spec] * 9,
            out_specs=(hbm_spec,) * 6,
            scratch_shapes=[
                pltpu.VMEM((parts, ms // parts, ml), F32), pltpu.VMEM((parts, ml // parts, ms), F32),
                pltpu.VMEM((2, layers, ms), F32), pltpu.VMEM((2, layers, ml), F32),
                dma((parts,)), dma((parts,)), dma((4,)),
            ],
            compiler_params=pltpu.CompilerParams(vmem_limit_bytes=VMEM_GRANT),
            name='write',
        )(*kept)

    return jax.shard_map(local_step, mesh=mesh, in_specs=(P(), tile_in, lane_row, lane_col, vec_row, vec_col, tile_out, lane_col, lane_row, vec_col, vec_row), out_specs=(tile_in, vec_row, vec_col, tile_out, vec_col, vec_row), check_vma=False)
```

```python
import functools

import jax
import jax.numpy as jnp
from jax import lax
from jax.experimental import pallas as pl
from jax.experimental.pallas import tpu as pltpu
from jax.sharding import PartitionSpec as P

EPS_ONE = 1e-30
EPS_TWO = 1e-3
LANE = 128
CHUNK = 1280
WSTEPS = 32
MESH = pl.DeviceIdType.MESH
F32 = jnp.float32
VMEM_GRANT = 20 * 2 ** 20


def tree(items):
    while len(items) > 1:
        items = [items[k] + items[k + 1] if k + 1 < len(items) else items[k] for k in range(0, len(items), 2)]
    return items[0]


def total(value):
    return jnp.sum(jnp.sum(value, axis=1, keepdims=True), axis=0, keepdims=True)


def stats_kernel(dims, hyper_hbm, w_in, x_in, dy_in, row_in, col_in, w_out, x_out, dy_out, row_out, col_out,
                 grad_lo, grad_hi, wv_in, wv_out, short_new, long_new, short_scale, long_scale, step_size,
                 act_s, act_l, lhs_t, old_s_in, old_l_in, old_s_out, old_l_out, short_old, long_old,
                 long_buf, short_buf, upd_buf, wsq_buf, racc, cacc, linv, pack, wpack, hyper_ref,
                 act_sem, w_sem, old_sem, long_send, long_recv, short_send, short_recv, fin_send, fin_recv):
    n_col, n_row, layers, ms, ml, d_model, d_hidden = dims
    n_dev = n_col * n_row
    half = layers // 2
    sch, lch = ms // LANE, ml // LANE
    my_col = lax.axis_index('col')
    my_row = lax.axis_index('row')
    me = my_col * n_row + my_row

    def act_copies(layer, kind):
        slot = 2 * lax.rem(layer, 2) + kind
        src_s = (x_in, dy_out)[kind]
        src_l = (dy_in, x_out)[kind]
        copies = [pltpu.make_async_copy(src_s.at[layer], act_s.at[slot], act_sem.at[slot, 0])]
        for c in range(ml // CHUNK):
            cols = pl.ds(c * CHUNK, CHUNK)
            copies.append(pltpu.make_async_copy(
                src_l.at[layer, :, cols], act_l.at[slot, :, cols], act_sem.at[slot, 1 + c]))
        return copies

    def w_copy(layer, kind):
        src = (w_in, w_out)[kind]
        dst = (wv_in, wv_out)[kind]
        return pltpu.make_async_copy(src.at[layer], dst.at[layer], w_sem.at[layer, kind])

    old_copies = [pltpu.make_async_copy(src, dst, old_sem.at[idx]) for idx, (src, dst) in enumerate(
        ((row_in, old_s_in), (col_in, old_l_in), (col_out, old_s_out), (row_out, old_l_out), (hyper_hbm, hyper_ref)))]

    for layer in range(2):
        for kind in range(2):
            for copy in act_copies(layer, kind):
                copy.start()
    for copy in old_copies:
        copy.start()
    for layer in range(layers):
        for kind in range(2):
            w_copy(layer, kind).start(priority=1)

    barrier = pltpu.get_barrier_semaphore()

    def peer_of(step):
        lin = lax.rem(me + step, n_dev)
        return (lin // n_row, lax.rem(lin, n_row))

    for step in range(1, n_dev):
        pl.semaphore_signal(barrier, inc=1, device_id=peer_of(step), device_id_type=MESH)

    pack[...] = jnp.zeros_like(pack)
    wpack[...] = jnp.zeros_like(wpack)

    def long_copy(mat, step):
        peer = lax.rem(my_row + step, n_row)
        return pltpu.make_async_remote_copy(
            src_ref=long_buf.at[mat, my_row], dst_ref=long_buf.at[mat, my_row],
            send_sem=long_send.at[mat], recv_sem=long_recv.at[mat],
            device_id=(my_col, peer), device_id_type=MESH)

    def short_copy(mat):
        return pltpu.make_async_remote_copy(
            src_ref=short_buf.at[mat, my_col], dst_ref=short_buf.at[mat, my_col],
            send_sem=short_send.at[mat], recv_sem=short_recv.at[mat],
            device_id=(n_col - 1 - my_col, my_row), device_id_type=MESH)

    def long_others(mat, sem):
        ref = long_buf.at[mat, pl.ds(0, n_row - 1)]
        return pltpu.make_async_copy(ref, ref, sem.at[mat])

    def fin_copy(buf, idx, step):
        return pltpu.make_async_remote_copy(
            src_ref=buf.at[me], dst_ref=buf.at[me], send_sem=fin_send.at[idx], recv_sem=fin_recv.at[idx],
            device_id=peer_of(step), device_id_type=MESH)

    def fin_others(buf, sem):
        ref = buf.at[pl.ds(0, n_dev - 1)]
        return pltpu.make_async_copy(ref, ref, sem)

    def put(where, lane, value):
        at = lax.broadcasted_iota(jnp.int32, (1, LANE), 1) == lane
        where[...] += jnp.where(at, value, 0.0)

    def dot_part(grad, base, mat, slot, c):
        cols = slice(c * CHUNK, (c + 1) * CHUNK)
        g = jnp.dot(lhs_t[...], act_l[slot, :, cols], preferred_element_type=F32)
        grad[mat - base, :, cols] = g
        sq = g * g
        part = tree([sq[:, j * LANE:(j + 1) * LANE] for j in range(CHUNK // LANE)])
        if c == 0:
            racc[...] = part
        else:
            racc[...] += part
        cacc[:, cols] = jnp.sum(sq.reshape(ms // 8, 8, CHUNK), axis=0)

    def upd_part(grad, base, mat, c):
        cols = slice(c * CHUNK, (c + 1) * CHUNK)
        acc = jnp.zeros((8, CHUNK), F32)
        for r in range(0, ms, 8):
            u = grad[mat - base, r:r + 8, cols] * jnp.tile(short_scale[mat, r:r + 8, :], (1, CHUNK // LANE))
            acc = acc + u * u
        first = c * CHUNK // LANE
        return tree([acc[:, j * LANE:(j + 1) * LANE] * linv[first + j:first + j + 1, :] for j in range(CHUNK // LANE)])

    def stats(layer, kind):
        mat = 2 * layer + kind
        long_others(mat, long_recv).wait()
        short_copy(mat).wait_recv()
        beta_two = hyper_ref[0]
        lsum = tree([long_buf[mat, dev] for dev in range(n_row)])
        ssum = tree([short_buf[mat, dev] for dev in range(n_col)])
        lnew = beta_two * long_old[mat] + (1.0 - beta_two) * (lsum * (1.0 / d_model) + EPS_ONE)
        snew = beta_two * short_old[mat] + (1.0 - beta_two) * (ssum * (1.0 / d_hidden) + EPS_ONE)
        long_new[mat] = lnew
        short_new[mat] = snew
        if kind == 0:
            rho = total(snew)
            rs = lax.rsqrt(snew / (rho * (1.0 / ms)))
            rl = lax.rsqrt(lnew)
        else:
            rho = total(lnew)
            rs = lax.rsqrt(snew)
            rl = lax.rsqrt(lnew / (rho * (1.0 / ml)))
        long_scale[mat] = rl
        linv[...] = rl * rl
        for j in range(sch):
            short_scale[mat, j * LANE:(j + 1) * LANE, :] = jnp.broadcast_to(rs[j:j + 1, :], (LANE, LANE)).T
        put(pack, mat + 2 * layers, rho)

    def send(mat):
        for j in range(lch):
            long_buf[mat, my_row, j:j + 1, :] = jnp.sum(cacc[:, j * LANE:(j + 1) * LANE], axis=0, keepdims=True)
        for j in range(sch):
            part = racc[j * LANE:(j + 1) * LANE, :].T
            short_buf[mat, my_col, j:j + 1, :] = jnp.sum(part, axis=0, keepdims=True)
        for step in range(1, n_row):
            long_copy(mat, step).start()
        short_copy(mat).start()

    def form_layer(layer, with_upd, layer_is_first=False):
        for kind in range(2):
            mat = 2 * layer + kind
            slot = 2 * lax.rem(layer, 2) + kind
            copies = act_copies(layer, kind)
            early = layer_is_first and kind == 0
            for copy in copies[:2] if early else copies:
                copy.wait()
            if with_upd:
                stats(layer - half, kind)
            lhs_t[...] = act_s[slot].T
            acc = []
            for c in range(ml // CHUNK):
                if c and early:
                    copies[1 + c].wait()
                if with_upd:
                    acc.append(upd_part(grad_lo, 0, mat - 2 * half, c))
                dot_part(*((grad_hi, 2 * half) if with_upd else (grad_lo, 0)), mat, slot, c)
            if with_upd:
                put(pack, mat - 2 * half, total(tree(acc)))
            else:
                for copy in act_copies(layer + half, kind):
                    copy.start()
            if early:
                pl.semaphore_wait(barrier, n_dev - 1)
            send(mat)

    def spread_old():
        for copy in old_copies:
            copy.wait()
        for kind, (src_s, src_l) in enumerate(((old_s_in, old_l_in), (old_s_out, old_l_out))):
            for each in range(layers):
                for j in range(sch):
                    short_old[2 * each + kind, j:j + 1, :] = src_s[each:each + 1, j * LANE:(j + 1) * LANE]
                for j in range(lch):
                    long_old[2 * each + kind, j:j + 1, :] = src_l[each:each + 1, j * LANE:(j + 1) * LANE]

    def first_half(layer, carry):
        form_layer(layer, False)
        return carry

    def second_half(layer, carry):
        form_layer(layer, True)
        return carry

    def upd_tail(layer, carry):
        for kind in range(2):
            mat = 2 * layer + kind
            stats(layer, kind)
            put(pack, mat, total(tree([upd_part(grad_hi, 2 * half, mat, c) for c in range(ml // CHUNK)])))
        return carry

    def weight_sq(layer, kind):
        w_copy(layer, kind).wait()
        ref = (wv_in, wv_out)[kind]
        rows, cols = ref.shape[1:]
        slab = max(8, 80 * LANE // cols // 8 * 8)
        width = min(cols, 10 * LANE)
        trip = WSTEPS * slab

        def chunk(t, acc):
            for step in range(WSTEPS):
                at = pl.ds(pl.multiple_of(t * trip + step * slab, 8), slab)
                for c in range(0, cols, width):
                    v = ref[layer, at, c:c + width]
                    acc = acc + v * v
            return acc

        acc = lax.fori_loop(0, rows // trip, chunk, jnp.zeros((slab, width), F32))
        acc = tree([acc[:, j * LANE:(j + 1) * LANE] for j in range(width // LANE)])
        put(wpack, 2 * layer + kind, total(tree([acc[j:j + 8] for j in range(0, slab, 8)])))

    def weights(layer, carry):
        for kind in range(2):
            weight_sq(layer, kind)
        return carry

    form_layer(0, False, True)
    spread_old()
    lax.fori_loop(1, half, first_half, 0)
    lax.fori_loop(half, layers, second_half, 0)
    lax.fori_loop(0, 2, weights, 0)
    lax.fori_loop(2, 3, upd_tail, 0)
    lax.fori_loop(2, 3, weights, 0)
    lax.fori_loop(3, 4, upd_tail, 0)
    upd_buf[me] = pack[...]
    for step in range(1, n_dev):
        fin_copy(upd_buf, 0, step).start()

    lax.fori_loop(3, 4, weights, 0)
    wsq_buf[me] = wpack[...]
    for step in range(1, n_dev):
        fin_copy(wsq_buf, 1, step).start()

    for mat in range(2 * layers):
        long_others(mat, long_send).wait()
        short_copy(mat).wait_send()
    fin_others(upd_buf, fin_send.at[0]).wait()
    fin_others(upd_buf, fin_recv.at[0]).wait()
    lane = lax.broadcasted_iota(jnp.int32, (1, LANE), 1)
    is_in = lax.rem(lane, 2) == 0
    valid = lane < 2 * layers
    shift = LANE - 2 * layers
    rho_sum = pltpu.roll(tree([upd_buf[dev] for dev in range(n_dev)]), shift, 1)
    row_mean = rho_sum * jnp.where(is_in, 1.0 / (n_col * d_model), 1.0 / (n_row * d_hidden))
    row_mean = jnp.where(valid, row_mean, 1.0)
    per_block = jnp.where(is_in, 1.0 / ms, 1.0 / ml)

    def ratio(rho):
        return row_mean / jnp.where(valid, pltpu.roll(rho, shift, 1) * per_block, 1.0)

    upd_sq = tree([upd_buf[dev] * ratio(upd_buf[dev]) for dev in range(n_dev)])
    n_total = float(d_model * d_hidden)
    upd_rms = jnp.sqrt(jnp.where(valid, upd_sq, 0.0) * (1.0 / n_total))
    before_w = hyper_ref[1] * jnp.sqrt(ratio(pack[...])) / jnp.maximum(1.0, upd_rms / hyper_ref[2])

    fin_others(wsq_buf, fin_send.at[1]).wait()
    fin_others(wsq_buf, fin_recv.at[1]).wait()
    w_sq = tree([wsq_buf[dev] for dev in range(n_dev)])
    w_rms = jnp.sqrt(w_sq * (1.0 / n_total))
    size = before_w * jnp.maximum(EPS_TWO, w_rms)
    step_size[...] = jnp.broadcast_to(size, (LANE, LANE)).T[:2 * layers, :]


def write_kernel(dims, grad_lo, grad_hi, wv_in, wv_out, short_new, long_new, short_scale, long_scale, step_size,
                 w_in_new, row_in_new, col_in_new, w_out_new, row_out_new, col_out_new,
                 stage_in, stage_out, vec_s, vec_l, sem_in, sem_out, sem_vec):
    layers, ms, ml, parts = dims
    half = layers // 2
    sch, lch = ms // LANE, ml // LANE
    rows_in, rows_out = ms // parts, ml // parts

    vec_copies = [pltpu.make_async_copy(src, dst, sem_vec.at[idx]) for idx, (src, dst) in enumerate(
        ((vec_s.at[0], row_in_new), (vec_l.at[0], col_in_new), (vec_s.at[1], col_out_new), (vec_l.at[1], row_out_new)))]

    def out_copy(layer, kind, part):
        if kind == 0:
            rows = pl.ds(pl.multiple_of(part * rows_in, rows_in), rows_in)
            return pltpu.make_async_copy(stage_in.at[part], w_in_new.at[layer, rows], sem_in.at[part])
        rows = pl.ds(pl.multiple_of(part * rows_out, rows_out), rows_out)
        return pltpu.make_async_copy(stage_out.at[part], w_out_new.at[layer, rows], sem_out.at[part])

    def one_part(layer, grad, mat, part):
        @pl.when(layer > 0)
        def _():
            for kind in range(2):
                out_copy(layer, kind, part).wait()

        rows = pl.ds(pl.multiple_of(part * rows_in, rows_in), rows_in)
        p_out = short_scale[2 * layer + 1] * step_size[pl.ds(2 * layer + 1, 1), :]
        p_in = short_scale[2 * layer, rows, :] * step_size[pl.ds(2 * layer, 1), :]
        per_row = rows_out // LANE
        for h in range(per_row):
            j = part * per_row + h
            cols = pl.ds(pl.multiple_of(j * LANE, LANE), LANE)
            u = grad[mat + 1, :, cols] * p_out * long_scale[2 * layer + 1, pl.ds(j, 1), :]
            stage_out[part, h * LANE:(h + 1) * LANE, :] = wv_out[layer, cols, :] - u.T
            for j in range(h * (lch // per_row), (h + 1) * (lch // per_row)):
                cols = slice(j * LANE, (j + 1) * LANE)
                u = grad[mat, rows, cols] * p_in * long_scale[2 * layer, j:j + 1, :]
                stage_in[part, :, cols] = wv_in[layer, rows, cols] - u
        for kind in range(2):
            out_copy(layer, kind, part).start()

    def loop(base, grad):
        def one(t, carry):
            layer = base + t // parts
            one_part(layer, grad, 2 * (t // parts), lax.rem(t, parts))
            return carry

        lax.fori_loop(0, half * parts, one, 0)

    loop(0, grad_lo)
    for each in range(layers):
        for kind in range(2):
            mat = 2 * each + kind
            for j in range(sch):
                vec_s[kind, each:each + 1, j * LANE:(j + 1) * LANE] = short_new[mat, j:j + 1, :]
            for j in range(lch):
                vec_l[kind, each:each + 1, j * LANE:(j + 1) * LANE] = long_new[mat, j:j + 1, :]
    for copy in vec_copies:
        copy.start()
    loop(half, grad_hi)
    for kind in range(2):
        for part in range(parts):
            out_copy(layers - 1, kind, part).wait()
    for copy in vec_copies:
        copy.wait()


def solution(mesh):
    n_col = mesh.shape['col']
    n_row = mesh.shape['row']
    tile_in = P(None, 'row', 'col')
    tile_out = P(None, 'col', 'row')
    lane_row = P(None, None, 'row')
    lane_col = P(None, None, 'col')
    vec_row = P(None, 'row')
    vec_col = P(None, 'col')

    def local_step(hyper_params, w_in, x_in, dy_in, row_in, col_in, w_out, x_out, dy_out, row_out, col_out):
        layers, ms, ml = w_in.shape
        tokens = x_in.shape[1]
        mats = 2 * layers
        sch, lch = ms // LANE, ml // LANE
        n_dev = n_col * n_row
        d_model, d_hidden = ms * n_row, ml * n_col
        hbm_spec = pl.BlockSpec(memory_space=pltpu.HBM)
        vmem_spec = pl.BlockSpec(memory_space=pltpu.VMEM)
        dims = (n_col, n_row, layers, ms, ml, d_model, d_hidden)
        bf16 = jnp.bfloat16
        dma = pltpu.SemaphoreType.DMA
        kept = pl.pallas_call(
            functools.partial(stats_kernel, dims),
            out_shape=(pltpu.VMEM((layers, ms, ml), F32), pltpu.VMEM((layers, ms, ml), F32),
                       pltpu.VMEM((layers, ms, ml), F32), pltpu.VMEM((layers, ml, ms), F32),
                       pltpu.VMEM((mats, sch, LANE), F32), pltpu.VMEM((mats, lch, LANE), F32),
                       pltpu.VMEM((mats, ms, LANE), F32), pltpu.VMEM((mats, lch, LANE), F32),
                       pltpu.VMEM((mats, LANE), F32)),
            in_specs=[hbm_spec] * 11,
            out_specs=(vmem_spec,) * 9,
            scratch_shapes=[
                pltpu.VMEM((4, tokens, ms), bf16), pltpu.VMEM((4, tokens, ml), bf16),
                pltpu.VMEM((ms, tokens), bf16),
                pltpu.VMEM((layers, ms), F32), pltpu.VMEM((layers, ml), F32),
                pltpu.VMEM((layers, ms), F32), pltpu.VMEM((layers, ml), F32),
                pltpu.VMEM((mats, sch, LANE), F32), pltpu.VMEM((mats, lch, LANE), F32),
                pltpu.VMEM((mats, n_row, lch, LANE), F32), pltpu.VMEM((mats, n_col, sch, LANE), F32),
                pltpu.VMEM((n_dev, 1, LANE), F32), pltpu.VMEM((n_dev, 1, LANE), F32),
                pltpu.VMEM((ms, LANE), F32), pltpu.VMEM((8, ml), F32),
                pltpu.VMEM((lch, LANE), F32), pltpu.VMEM((1, LANE), F32), pltpu.VMEM((1, LANE), F32),
                pltpu.SMEM((3,), F32),
                dma((4, 1 + ml // CHUNK)), dma((layers, 2)), dma((5,)),
                dma((mats,)), dma((mats,)), dma((mats,)), dma((mats,)), dma((2,)), dma((2,)),
            ],
            compiler_params=pltpu.CompilerParams(
                collective_id=0, has_side_effects=True, vmem_limit_bytes=VMEM_GRANT),
            name='stats',
        )(*(pltpu.with_memory_space_constraint(item, pltpu.HBM) for item in (
            hyper_params, w_in, x_in, dy_in, row_in, col_in, w_out, x_out, dy_out, row_out, col_out)))
        kept = tuple(pltpu.with_memory_space_constraint(item, pltpu.VMEM) for item in kept)
        parts = 4
        return pl.pallas_call(
            functools.partial(write_kernel, (layers, ms, ml, parts)),
            out_shape=tuple(jax.ShapeDtypeStruct(item.shape, F32) for item in (
                w_in, row_in, col_in, w_out, row_out, col_out)),
            in_specs=[vmem_spec] * 9,
            out_specs=(hbm_spec,) * 6,
            scratch_shapes=[
                pltpu.VMEM((parts, ms // parts, ml), F32), pltpu.VMEM((parts, ml // parts, ms), F32),
                pltpu.VMEM((2, layers, ms), F32), pltpu.VMEM((2, layers, ml), F32),
                dma((parts,)), dma((parts,)), dma((4,)),
            ],
            compiler_params=pltpu.CompilerParams(vmem_limit_bytes=VMEM_GRANT),
            name='write',
        )(*kept)

    return jax.shard_map(local_step, mesh=mesh, in_specs=(P(), tile_in, lane_row, lane_col, vec_row, vec_col, tile_out, lane_col, lane_row, vec_col, vec_row), out_specs=(tile_in, vec_row, vec_col, tile_out, vec_col, vec_row), check_vma=False)
```

```python
import functools

import jax
import jax.numpy as jnp
from jax import lax
from jax.experimental import pallas as pl
from jax.experimental.pallas import tpu as pltpu
from jax.sharding import PartitionSpec as P

EPS_ONE = 1e-30
EPS_TWO = 1e-3
LANE = 128
CHUNK = 512
WSTEPS = 32
MESH = pl.DeviceIdType.MESH
F32 = jnp.float32
VMEM_GRANT = 20 * 2 ** 20


def tree(items):
    while len(items) > 1:
        items = [items[k] + items[k + 1] if k + 1 < len(items) else items[k] for k in range(0, len(items), 2)]
    return items[0]


def total(value):
    return jnp.sum(jnp.sum(value, axis=1, keepdims=True), axis=0, keepdims=True)


def stats_kernel(dims, hyper_hbm, w_in, x_in, dy_in, row_in, col_in, w_out, x_out, dy_out, row_out, col_out,
                 grad_lo, grad_hi, wv_in, wv_out, short_new, long_new, short_scale, long_scale, step_size,
                 act_s, act_l, lhs_t, old_s_in, old_l_in, old_s_out, old_l_out, short_old, long_old,
                 long_buf, short_buf, upd_buf, wsq_buf, racc, cacc, linv, pack, wpack, hyper_ref,
                 act_sem, w_sem, old_sem, long_send, long_recv, short_send, short_recv, fin_send, fin_recv):
    n_col, n_row, layers, ms, ml, d_model, d_hidden = dims
    n_dev = n_col * n_row
    half = layers // 2
    sch, lch = ms // LANE, ml // LANE
    my_col = lax.axis_index('col')
    my_row = lax.axis_index('row')
    me = my_col * n_row + my_row

    def act_copies(layer, kind):
        slot = 2 * lax.rem(layer, 2) + kind
        src_s = (x_in, dy_out)[kind]
        src_l = (dy_in, x_out)[kind]
        copies = [pltpu.make_async_copy(src_s.at[layer], act_s.at[slot], act_sem.at[slot, 0])]
        for c in range(ml // CHUNK):
            cols = pl.ds(c * CHUNK, CHUNK)
            copies.append(pltpu.make_async_copy(
                src_l.at[layer, :, cols], act_l.at[slot, :, cols], act_sem.at[slot, 1 + c]))
        return copies

    def w_copy(layer, kind):
        src = (w_in, w_out)[kind]
        dst = (wv_in, wv_out)[kind]
        return pltpu.make_async_copy(src.at[layer], dst.at[layer], w_sem.at[layer, kind])

    old_copies = [pltpu.make_async_copy(src, dst, old_sem.at[idx]) for idx, (src, dst) in enumerate(
        ((row_in, old_s_in), (col_in, old_l_in), (col_out, old_s_out), (row_out, old_l_out), (hyper_hbm, hyper_ref)))]

    for layer in range(2):
        for kind in range(2):
            for copy in act_copies(layer, kind):
                copy.start()
    for copy in old_copies:
        copy.start()
    for layer in range(layers):
        for kind in range(2):
            w_copy(layer, kind).start(priority=1)

    barrier = pltpu.get_barrier_semaphore()

    def peer_of(step):
        lin = lax.rem(me + step, n_dev)
        return (lin // n_row, lax.rem(lin, n_row))

    for step in range(1, n_dev):
        pl.semaphore_signal(barrier, inc=1, device_id=peer_of(step), device_id_type=MESH)

    pack[...] = jnp.zeros_like(pack)
    wpack[...] = jnp.zeros_like(wpack)

    def long_copy(mat, step):
        peer = lax.rem(my_row + step, n_row)
        return pltpu.make_async_remote_copy(
            src_ref=long_buf.at[mat, my_row], dst_ref=long_buf.at[mat, my_row],
            send_sem=long_send.at[mat], recv_sem=long_recv.at[mat],
            device_id=(my_col, peer), device_id_type=MESH)

    def short_copy(mat):
        return pltpu.make_async_remote_copy(
            src_ref=short_buf.at[mat, my_col], dst_ref=short_buf.at[mat, my_col],
            send_sem=short_send.at[mat], recv_sem=short_recv.at[mat],
            device_id=(n_col - 1 - my_col, my_row), device_id_type=MESH)

    def long_others(mat, sem):
        ref = long_buf.at[mat, pl.ds(0, n_row - 1)]
        return pltpu.make_async_copy(ref, ref, sem.at[mat])

    def fin_copy(buf, idx, step):
        return pltpu.make_async_remote_copy(
            src_ref=buf.at[me], dst_ref=buf.at[me], send_sem=fin_send.at[idx], recv_sem=fin_recv.at[idx],
            device_id=peer_of(step), device_id_type=MESH)

    def fin_others(buf, sem):
        ref = buf.at[pl.ds(0, n_dev - 1)]
        return pltpu.make_async_copy(ref, ref, sem)

    def put(where, lane, value):
        at = lax.broadcasted_iota(jnp.int32, (1, LANE), 1) == lane
        where[...] += jnp.where(at, value, 0.0)

    def dot_part(grad, base, mat, slot, c):
        cols = slice(c * CHUNK, (c + 1) * CHUNK)
        g = jnp.dot(lhs_t[...], act_l[slot, :, cols], preferred_element_type=F32)
        grad[mat - base, :, cols] = g
        sq = g * g
        part = tree([sq[:, j * LANE:(j + 1) * LANE] for j in range(CHUNK // LANE)])
        if c == 0:
            racc[...] = part
        else:
            racc[...] += part
        cacc[:, cols] = jnp.sum(sq.reshape(ms // 8, 8, CHUNK), axis=0)

    def upd_part(grad, base, mat, c):
        cols = slice(c * CHUNK, (c + 1) * CHUNK)
        acc = jnp.zeros((8, CHUNK), F32)
        for r in range(0, ms, 8):
            u = grad[mat - base, r:r + 8, cols] * jnp.tile(short_scale[mat, r:r + 8, :], (1, CHUNK // LANE))
            acc = acc + u * u
        first = c * CHUNK // LANE
        return tree([acc[:, j * LANE:(j + 1) * LANE] * linv[first + j:first + j + 1, :] for j in range(CHUNK // LANE)])

    def stats(layer, kind):
        mat = 2 * layer + kind
        long_others(mat, long_recv).wait()
        short_copy(mat).wait_recv()
        beta_two = hyper_ref[0]
        lsum = tree([long_buf[mat, dev] for dev in range(n_row)])
        ssum = tree([short_buf[mat, dev] for dev in range(n_col)])
        lnew = beta_two * long_old[mat] + (1.0 - beta_two) * (lsum * (1.0 / d_model) + EPS_ONE)
        snew = beta_two * short_old[mat] + (1.0 - beta_two) * (ssum * (1.0 / d_hidden) + EPS_ONE)
        long_new[mat] = lnew
        short_new[mat] = snew
        if kind == 0:
            rho = total(snew)
            rs = lax.rsqrt(snew / (rho * (1.0 / ms)))
            rl = lax.rsqrt(lnew)
        else:
            rho = total(lnew)
            rs = lax.rsqrt(snew)
            rl = lax.rsqrt(lnew / (rho * (1.0 / ml)))
        long_scale[mat] = rl
        linv[...] = rl * rl
        for j in range(sch):
            short_scale[mat, j * LANE:(j + 1) * LANE, :] = jnp.broadcast_to(rs[j:j + 1, :], (LANE, LANE)).T
        put(pack, mat + 2 * layers, rho)

    def send(mat):
        for j in range(lch):
            long_buf[mat, my_row, j:j + 1, :] = jnp.sum(cacc[:, j * LANE:(j + 1) * LANE], axis=0, keepdims=True)
        for j in range(sch):
            part = racc[j * LANE:(j + 1) * LANE, :].T
            short_buf[mat, my_col, j:j + 1, :] = jnp.sum(part, axis=0, keepdims=True)
        for step in range(1, n_row):
            long_copy(mat, step).start()
        short_copy(mat).start()

    def form_layer(layer, with_upd, layer_is_first=False):
        for kind in range(2):
            mat = 2 * layer + kind
            slot = 2 * lax.rem(layer, 2) + kind
            copies = act_copies(layer, kind)
            early = layer_is_first and kind == 0
            for copy in copies[:2] if early else copies:
                copy.wait()
            if with_upd:
                stats(layer - half, kind)
            lhs_t[...] = act_s[slot].T
            acc = []
            for c in range(ml // CHUNK):
                if c and early:
                    copies[1 + c].wait()
                if with_upd:
                    acc.append(upd_part(grad_lo, 0, mat - 2 * half, c))
                dot_part(*((grad_hi, 2 * half) if with_upd else (grad_lo, 0)), mat, slot, c)
            if with_upd:
                put(pack, mat - 2 * half, total(tree(acc)))
            else:
                for copy in act_copies(layer + half, kind):
                    copy.start()
            if early:
                pl.semaphore_wait(barrier, n_dev - 1)
            send(mat)

    def spread_old():
        for copy in old_copies:
            copy.wait()
        for kind, (src_s, src_l) in enumerate(((old_s_in, old_l_in), (old_s_out, old_l_out))):
            for each in range(layers):
                for j in range(sch):
                    short_old[2 * each + kind, j:j + 1, :] = src_s[each:each + 1, j * LANE:(j + 1) * LANE]
                for j in range(lch):
                    long_old[2 * each + kind, j:j + 1, :] = src_l[each:each + 1, j * LANE:(j + 1) * LANE]

    def first_half(layer, carry):
        form_layer(layer, False)
        return carry

    def second_half(layer, carry):
        form_layer(layer, True)
        return carry

    def upd_tail(layer, carry):
        for kind in range(2):
            mat = 2 * layer + kind
            stats(layer, kind)
            put(pack, mat, total(tree([upd_part(grad_hi, 2 * half, mat, c) for c in range(ml // CHUNK)])))
        return carry

    def weight_sq(layer, kind):
        w_copy(layer, kind).wait()
        ref = (wv_in, wv_out)[kind]
        rows, cols = ref.shape[1:]
        slab = max(8, 80 * LANE // cols // 8 * 8)
        width = min(cols, 10 * LANE)
        trip = WSTEPS * slab

        def chunk(t, acc):
            for step in range(WSTEPS):
                at = pl.ds(pl.multiple_of(t * trip + step * slab, 8), slab)
                for c in range(0, cols, width):
                    v = ref[layer, at, c:c + width]
                    acc = acc + v * v
            return acc

        acc = lax.fori_loop(0, rows // trip, chunk, jnp.zeros((slab, width), F32))
        acc = tree([acc[:, j * LANE:(j + 1) * LANE] for j in range(width // LANE)])
        put(wpack, 2 * layer + kind, total(tree([acc[j:j + 8] for j in range(0, slab, 8)])))

    def weights(layer, carry):
        for kind in range(2):
            weight_sq(layer, kind)
        return carry

    form_layer(0, False, True)
    spread_old()
    lax.fori_loop(1, half, first_half, 0)
    lax.fori_loop(half, layers, second_half, 0)
    lax.fori_loop(0, 2, weights, 0)
    lax.fori_loop(2, 3, upd_tail, 0)
    lax.fori_loop(2, 3, weights, 0)
    lax.fori_loop(3, 4, upd_tail, 0)
    upd_buf[me] = pack[...]
    for step in range(1, n_dev):
        fin_copy(upd_buf, 0, step).start()

    lax.fori_loop(3, 4, weights, 0)
    wsq_buf[me] = wpack[...]
    for step in range(1, n_dev):
        fin_copy(wsq_buf, 1, step).start()

    for mat in range(2 * layers):
        long_others(mat, long_send).wait()
        short_copy(mat).wait_send()
    fin_others(upd_buf, fin_send.at[0]).wait()
    fin_others(upd_buf, fin_recv.at[0]).wait()
    lane = lax.broadcasted_iota(jnp.int32, (1, LANE), 1)
    is_in = lax.rem(lane, 2) == 0
    valid = lane < 2 * layers
    shift = LANE - 2 * layers
    rho_sum = pltpu.roll(tree([upd_buf[dev] for dev in range(n_dev)]), shift, 1)
    row_mean = rho_sum * jnp.where(is_in, 1.0 / (n_col * d_model), 1.0 / (n_row * d_hidden))
    row_mean = jnp.where(valid, row_mean, 1.0)
    per_block = jnp.where(is_in, 1.0 / ms, 1.0 / ml)

    def ratio(rho):
        return row_mean / jnp.where(valid, pltpu.roll(rho, shift, 1) * per_block, 1.0)

    upd_sq = tree([upd_buf[dev] * ratio(upd_buf[dev]) for dev in range(n_dev)])
    n_total = float(d_model * d_hidden)
    upd_rms = jnp.sqrt(jnp.where(valid, upd_sq, 0.0) * (1.0 / n_total))
    before_w = hyper_ref[1] * jnp.sqrt(ratio(pack[...])) / jnp.maximum(1.0, upd_rms / hyper_ref[2])

    fin_others(wsq_buf, fin_send.at[1]).wait()
    fin_others(wsq_buf, fin_recv.at[1]).wait()
    w_sq = tree([wsq_buf[dev] for dev in range(n_dev)])
    w_rms = jnp.sqrt(w_sq * (1.0 / n_total))
    size = before_w * jnp.maximum(EPS_TWO, w_rms)
    step_size[...] = jnp.broadcast_to(size, (LANE, LANE)).T[:2 * layers, :]


def write_kernel(dims, grad_lo, grad_hi, wv_in, wv_out, short_new, long_new, short_scale, long_scale, step_size,
                 w_in_new, row_in_new, col_in_new, w_out_new, row_out_new, col_out_new,
                 stage_in, stage_out, vec_s, vec_l, sem_in, sem_out, sem_vec):
    layers, ms, ml, parts = dims
    half = layers // 2
    sch, lch = ms // LANE, ml // LANE
    rows_in, rows_out = ms // parts, ml // parts

    vec_copies = [pltpu.make_async_copy(src, dst, sem_vec.at[idx]) for idx, (src, dst) in enumerate(
        ((vec_s.at[0], row_in_new), (vec_l.at[0], col_in_new), (vec_s.at[1], col_out_new), (vec_l.at[1], row_out_new)))]

    def out_copy(layer, kind, part):
        if kind == 0:
            rows = pl.ds(pl.multiple_of(part * rows_in, rows_in), rows_in)
            return pltpu.make_async_copy(stage_in.at[part], w_in_new.at[layer, rows], sem_in.at[part])
        rows = pl.ds(pl.multiple_of(part * rows_out, rows_out), rows_out)
        return pltpu.make_async_copy(stage_out.at[part], w_out_new.at[layer, rows], sem_out.at[part])

    def one_part(layer, grad, mat, part):
        @pl.when(layer > 0)
        def _():
            for kind in range(2):
                out_copy(layer, kind, part).wait()

        rows = pl.ds(pl.multiple_of(part * rows_in, rows_in), rows_in)
        p_out = short_scale[2 * layer + 1] * step_size[pl.ds(2 * layer + 1, 1), :]
        p_in = short_scale[2 * layer, rows, :] * step_size[pl.ds(2 * layer, 1), :]
        per_row = rows_out // LANE
        for h in range(per_row):
            j = part * per_row + h
            cols = pl.ds(pl.multiple_of(j * LANE, LANE), LANE)
            u = grad[mat + 1, :, cols] * p_out * long_scale[2 * layer + 1, pl.ds(j, 1), :]
            stage_out[part, h * LANE:(h + 1) * LANE, :] = wv_out[layer, cols, :] - u.T
            for j in range(h * (lch // per_row), (h + 1) * (lch // per_row)):
                cols = slice(j * LANE, (j + 1) * LANE)
                u = grad[mat, rows, cols] * p_in * long_scale[2 * layer, j:j + 1, :]
                stage_in[part, :, cols] = wv_in[layer, rows, cols] - u
        for kind in range(2):
            out_copy(layer, kind, part).start()

    def loop(base, grad):
        def one(t, carry):
            layer = base + t // parts
            one_part(layer, grad, 2 * (t // parts), lax.rem(t, parts))
            return carry

        lax.fori_loop(0, half * parts, one, 0)

    loop(0, grad_lo)
    for each in range(layers):
        for kind in range(2):
            mat = 2 * each + kind
            for j in range(sch):
                vec_s[kind, each:each + 1, j * LANE:(j + 1) * LANE] = short_new[mat, j:j + 1, :]
            for j in range(lch):
                vec_l[kind, each:each + 1, j * LANE:(j + 1) * LANE] = long_new[mat, j:j + 1, :]
    for copy in vec_copies:
        copy.start()
    loop(half, grad_hi)
    for kind in range(2):
        for part in range(parts):
            out_copy(layers - 1, kind, part).wait()
    for copy in vec_copies:
        copy.wait()


def solution(mesh):
    n_col = mesh.shape['col']
    n_row = mesh.shape['row']
    tile_in = P(None, 'row', 'col')
    tile_out = P(None, 'col', 'row')
    lane_row = P(None, None, 'row')
    lane_col = P(None, None, 'col')
    vec_row = P(None, 'row')
    vec_col = P(None, 'col')

    def local_step(hyper_params, w_in, x_in, dy_in, row_in, col_in, w_out, x_out, dy_out, row_out, col_out):
        layers, ms, ml = w_in.shape
        tokens = x_in.shape[1]
        mats = 2 * layers
        sch, lch = ms // LANE, ml // LANE
        n_dev = n_col * n_row
        d_model, d_hidden = ms * n_row, ml * n_col
        hbm_spec = pl.BlockSpec(memory_space=pltpu.HBM)
        vmem_spec = pl.BlockSpec(memory_space=pltpu.VMEM)
        dims = (n_col, n_row, layers, ms, ml, d_model, d_hidden)
        bf16 = jnp.bfloat16
        dma = pltpu.SemaphoreType.DMA
        kept = pl.pallas_call(
            functools.partial(stats_kernel, dims),
            out_shape=(pltpu.VMEM((layers, ms, ml), F32), pltpu.VMEM((layers, ms, ml), F32),
                       pltpu.VMEM((layers, ms, ml), F32), pltpu.VMEM((layers, ml, ms), F32),
                       pltpu.VMEM((mats, sch, LANE), F32), pltpu.VMEM((mats, lch, LANE), F32),
                       pltpu.VMEM((mats, ms, LANE), F32), pltpu.VMEM((mats, lch, LANE), F32),
                       pltpu.VMEM((mats, LANE), F32)),
            in_specs=[hbm_spec] * 11,
            out_specs=(vmem_spec,) * 9,
            scratch_shapes=[
                pltpu.VMEM((4, tokens, ms), bf16), pltpu.VMEM((4, tokens, ml), bf16),
                pltpu.VMEM((ms, tokens), bf16),
                pltpu.VMEM((layers, ms), F32), pltpu.VMEM((layers, ml), F32),
                pltpu.VMEM((layers, ms), F32), pltpu.VMEM((layers, ml), F32),
                pltpu.VMEM((mats, sch, LANE), F32), pltpu.VMEM((mats, lch, LANE), F32),
                pltpu.VMEM((mats, n_row, lch, LANE), F32), pltpu.VMEM((mats, n_col, sch, LANE), F32),
                pltpu.VMEM((n_dev, 1, LANE), F32), pltpu.VMEM((n_dev, 1, LANE), F32),
                pltpu.VMEM((ms, LANE), F32), pltpu.VMEM((8, ml), F32),
                pltpu.VMEM((lch, LANE), F32), pltpu.VMEM((1, LANE), F32), pltpu.VMEM((1, LANE), F32),
                pltpu.SMEM((3,), F32),
                dma((4, 1 + ml // CHUNK)), dma((layers, 2)), dma((5,)),
                dma((mats,)), dma((mats,)), dma((mats,)), dma((mats,)), dma((2,)), dma((2,)),
            ],
            compiler_params=pltpu.CompilerParams(
                collective_id=0, has_side_effects=True, vmem_limit_bytes=VMEM_GRANT),
            name='stats',
        )(*(pltpu.with_memory_space_constraint(item, pltpu.HBM) for item in (
            hyper_params, w_in, x_in, dy_in, row_in, col_in, w_out, x_out, dy_out, row_out, col_out)))
        kept = tuple(pltpu.with_memory_space_constraint(item, pltpu.VMEM) for item in kept)
        parts = 4
        return pl.pallas_call(
            functools.partial(write_kernel, (layers, ms, ml, parts)),
            out_shape=tuple(jax.ShapeDtypeStruct(item.shape, F32) for item in (
                w_in, row_in, col_in, w_out, row_out, col_out)),
            in_specs=[vmem_spec] * 9,
            out_specs=(hbm_spec,) * 6,
            scratch_shapes=[
                pltpu.VMEM((parts, ms // parts, ml), F32), pltpu.VMEM((parts, ml // parts, ms), F32),
                pltpu.VMEM((2, layers, ms), F32), pltpu.VMEM((2, layers, ml), F32),
                dma((parts,)), dma((parts,)), dma((4,)),
            ],
            compiler_params=pltpu.CompilerParams(vmem_limit_bytes=VMEM_GRANT),
            name='write',
        )(*kept)

    return jax.shard_map(local_step, mesh=mesh, in_specs=(P(), tile_in, lane_row, lane_col, vec_row, vec_col, tile_out, lane_col, lane_row, vec_col, vec_row), out_specs=(tile_in, vec_row, vec_col, tile_out, vec_col, vec_row), check_vma=False)
```
